32 devices in a mesh: gx: 8 (over z, y), gy: 4 (over x, core).
Axes of the slice: x: 2, y: 2, z: 4, core: 2. Of those that a mesh axis runs over, the one named last changes fastest.
Arguments:
- snapshots: bfloat16 [8, 8, 4, 2048, 512], P('gx', 'gy'), may hold values from -120 to 120
- basis: bfloat16 [8, 8, 4, 24, 2048], P('gx', 'gy'), may hold values from -0.0625 to 0.0625
- node_counts: int32 [8, 8], P('gx', 'gy'), may hold values from 1024 to 2048, as said below
- adjacency: int32 [8, 8, 3], P('gx', 'gy'), may hold values from 0 to 63, as said below
Outputs:
- operator: float32 [8, 8, 397, 24], P('gx', 'gy')
- reduced_states: float32 [8, 8, 24, 512], P('gx', 'gy')
The draws below stay inside these ranges and needn't reach their ends.
Inputs may be any that keep to these rules, and one draw needn't show every extreme that they name: Node slot n of subdomain g is live iff n < node_counts[g]; at least 1024 slots are live, and one subdomain has all 2048 live. Subdomain (row, col) has id row * 8 + col. Each row of adjacency holds 3 distinct ids other than its own subdomain's, each within one subdomain row and one subdomain column of it.
All inputs are finite; a program needn't handle non-finite values.
Results may differ from the reference program's by a relative error of at most 0.0003.
Values sent between devices are 32-bit elements; how exact they have to be, the bound alone decides.
A program may use at most 64 MiB of HBM per device.

```python
import jax
import jax.numpy as jnp
import numpy as np
from jax import lax

R = 24
NVAR = 4
K = 512
P_SIZE = 2048
NB = 3
GRID_R = 8
GRID_C = 8
NF = 397


def draw_node_counts(key, part):
    first, second = jax.random.split(jax.random.fold_in(key, 11))
    counts = jax.random.randint(first, (GRID_R * GRID_C,), P_SIZE // 2, P_SIZE + 1, dtype=jnp.int32)
    where_full = jax.random.randint(second, (), 0, GRID_R * GRID_C, dtype=jnp.int32)
    counts = jnp.where(jnp.arange(GRID_R * GRID_C, dtype=jnp.int32) == where_full, P_SIZE, counts)
    return counts.reshape(GRID_R, GRID_C).astype(jnp.int32)


def draw_adjacency(key, part):
    offsets = np.array([(a, b) for a in range(-1, 2) for b in range(-1, 2)], dtype=np.int32)
    rows = jnp.arange(GRID_R, dtype=jnp.int32)[:, None, None]
    cols = jnp.arange(GRID_C, dtype=jnp.int32)[None, :, None]
    near_rows = jnp.broadcast_to(rows + jnp.asarray(offsets[:, 0]), (GRID_R, GRID_C, 9))
    near_cols = jnp.broadcast_to(cols + jnp.asarray(offsets[:, 1]), (GRID_R, GRID_C, 9))
    inside = (near_rows >= 0) & (near_rows < GRID_R) & (near_cols >= 0) & (near_cols < GRID_C)
    itself = (near_rows == rows) & (near_cols == cols)
    scores = jax.random.randint(jax.random.fold_in(key, 13), (GRID_R, GRID_C, 9), 0, 1000, dtype=jnp.int32) * 16 + jnp.arange(9, dtype=jnp.int32)
    scores = jnp.where(inside & jnp.logical_not(itself), scores, -1)
    unused, picked = lax.top_k(scores, NB)
    chosen_rows = jnp.take_along_axis(near_rows, picked, axis=2)
    chosen_cols = jnp.take_along_axis(near_cols, picked, axis=2)
    return (chosen_rows * GRID_C + chosen_cols).astype(jnp.int32)


def draw_snapshots(key, part):
    keys = jax.random.split(jax.random.fold_in(key, 17), 3)
    shape = (GRID_R, GRID_C, NVAR, P_SIZE, K)
    ident = jnp.arange(GRID_R * GRID_C, dtype=jnp.float32).reshape(GRID_R, GRID_C) / max(GRID_R * GRID_C - 1, 1)
    var_scale = jnp.exp(jax.random.uniform(keys[0], (NVAR,), jnp.float32, jnp.log(0.5), jnp.log(4.0)))
    rough = jax.random.uniform(keys[1], (GRID_R, GRID_C, NVAR, P_SIZE, 1), jnp.float32, 0.5, 1.5)
    base = jnp.clip(jax.random.normal(keys[2], shape, jnp.float32), -6.0, 6.0)
    rise = 1.0 + 2.0 * ident
    values = base * rough * var_scale[None, None, :, None, None] * rise[:, :, None, None, None]
    return values.astype(jnp.bfloat16)


def shard_levels(rng, shape, shards, least, top_value):
    loudness, own = 1.0, jax.random.fold_in(rng, 6)
    for position, parts in shards:
        steps = jnp.exp(jax.random.uniform(jax.random.fold_in(own, position), (parts,), jnp.float32, least / len(shards), top_value / len(shards)))
        loudness = loudness * jnp.repeat(steps, shape[position] // parts).reshape([-1 if axis == position else 1 for axis in range(len(shape))])
    return loudness


def gaussian(own_key, shape, deviation, reach, cuts=(), kind=jnp.bfloat16):
    result = jax.random.normal(own_key, shape, jnp.float32) * deviation
    if len(cuts) > 0:
        result = shard_levels(own_key, shape, cuts, -0.22, 0.18) * result
    return jnp.clip(result, min=-reach, max=reach).astype(kind)


def setup_inputs(seed: int = 0) -> dict:
    seeds = jax.random.split(jax.random.key(seed), 5)
    return {
        "snapshots": draw_snapshots(jax.random.fold_in(seeds[4], 71), 0),
        "basis": gaussian(seeds[1], (GRID_R, GRID_C, NVAR, R, P_SIZE), (NVAR * P_SIZE) ** -0.5, 0.0625, ((0, 8), (1, 4))),
        "node_counts": draw_node_counts(jax.random.fold_in(seeds[4], 71), 0),
        "adjacency": draw_adjacency(jax.random.fold_in(seeds[4], 71), 0),
    }


beta_linear = 0.5
beta_quad = 0.5

def project_one(items):
    values, modes, count = items
    live = (jnp.arange(values.shape[1], dtype=jnp.int32) < count).astype(jnp.float32)
    masked = modes.astype(jnp.float32) * live[None, None, :]
    proj = jnp.einsum('vrp,vpk->vrk', masked, values.astype(jnp.float32), precision=lax.Precision.HIGHEST)
    valf = values.astype(jnp.float32)
    squares = lax.optimization_barrier(jnp.sum(valf * valf * live[None, :, None], axis=(1, 2)))
    return (proj, squares)

def build_features(state, near):
    ranks = state.shape[0]
    steps = state.shape[1]
    pieces = [jnp.ones((1, steps), jnp.float32), state, near.reshape(-1, steps)]
    for first in range(ranks):
        pieces.append(state[first:first + 1] * state[first:])
    return jnp.concatenate(pieces, axis=0)

def fit_one(state, near, reg_diag):
    feats = build_features(state, near)
    past = feats[:, :-1]
    gram = jnp.dot(past, past.T, precision=lax.Precision.HIGHEST) + jnp.diag(reg_diag)
    rhs = jnp.dot(past, state[:, 1:].T, precision=lax.Precision.HIGHEST)
    factor = jnp.linalg.cholesky(gram)
    middle = jax.scipy.linalg.solve_triangular(factor, rhs, lower=True)
    return jax.scipy.linalg.solve_triangular(factor, middle, lower=True, trans=1)

def reference(snapshots, basis, node_counts, adjacency):
    grid_rows, grid_cols = (snapshots.shape[0], snapshots.shape[1])
    total = grid_rows * grid_cols
    values = snapshots.reshape(total, NVAR, P_SIZE, K)
    modes = basis.reshape(total, NVAR, R, P_SIZE)
    counts = node_counts.reshape(total).astype(jnp.int32)
    proj, squares = lax.map(project_one, (values, modes, counts))
    nodes = jnp.sum(counts.astype(jnp.float32))
    scale = jnp.sqrt(lax.optimization_barrier(jnp.sum(squares, axis=0)) / (nodes * K) + 1e-06)
    states = lax.optimization_barrier(jnp.sum(proj / scale[None, :, None, None], axis=1))
    gnorm = jnp.sum(states * states) / (total * R * K)
    near = states[adjacency.reshape(total, NB).astype(jnp.int32)]
    nlin = 1 + R + NB * R
    nquad = R * (R + 1) // 2
    reg_diag = K * jnp.concatenate([jnp.full((nlin,), beta_linear, jnp.float32) * gnorm, jnp.full((nquad,), beta_quad, jnp.float32) * gnorm * gnorm])
    operator = lax.map(lambda items: fit_one(items[0], items[1], reg_diag), (states, near))
    return (operator.reshape(grid_rows, grid_cols, NF, R), states.reshape(grid_rows, grid_cols, R, K))
```

```python
import jax
import jax.numpy as jnp
from jax import lax
from jax.experimental import pallas as pl
from jax.experimental.pallas import tpu as pltpu
from jax.sharding import PartitionSpec as P

beta_linear = 0.5
beta_quad = 0.5
LANES = 128
SUB = 8


def spread_row(tile, row):
    return jnp.broadcast_to(tile[row : row + 1, :], tile.shape)


def spread_lane(tile, lane):
    return jnp.broadcast_to(tile[:, lane : lane + 1], tile.shape)


def split3(a):
    hi = a.astype(jnp.bfloat16)
    left = a - hi.astype(jnp.float32)
    mid = left.astype(jnp.bfloat16)
    low = (left - mid.astype(jnp.float32)).astype(jnp.bfloat16)
    return hi, mid, low


def as_left(parts):
    hi, mid, low = parts
    return jnp.concatenate([hi, mid, hi, mid, hi, low], axis=1)


def as_right(parts, axis=1):
    hi, mid, low = parts
    return jnp.concatenate([hi, mid, mid, hi, low, hi], axis=axis)


def dot_nt(a, b):
    return lax.dot_general(a, b, (((1,), (1,)), ((), ())), preferred_element_type=jnp.float32)


def dot_nn(a, b):
    return jnp.dot(a, b, preferred_element_type=jnp.float32)


def whiten(blocks):
    size = blocks[0].shape[0]
    sub = lax.broadcasted_iota(jnp.int32, (SUB, LANES), 0)
    lane = lax.broadcasted_iota(jnp.int32, (SUB, LANES), 1)
    count = len(blocks)
    tiles = [[b[r : r + SUB, :] for r in range(0, size, SUB)] for b in blocks]
    out = [[] for b in blocks]
    for p in range(size // SUB):
        base = p * SUB
        inside = (lane >= base) & (lane < base + SUB)
        unit = (lane - base == sub).astype(jnp.float32)
        cols = [[spread_lane(t[p], base + j) for j in range(SUB)] for t in tiles]
        here = [jnp.where(inside, unit, t[p]) for t in tiles]
        scaled = [jnp.zeros((SUB, LANES), jnp.float32) for t in tiles]
        for j in range(SUB):
            for s in range(count):
                col = cols[s][j]
                pivot = spread_row(col, j)
                inv = 1.0 / pivot
                row = spread_row(here[s], j)
                scaled[s] = jnp.where(sub == j, row * lax.rsqrt(pivot), scaled[s])
                row = row * inv
                here[s] = jnp.where(sub == j, row, here[s] - col * row)
                for i in range(j + 1, SUB):
                    row = spread_row(cols[s][i], j) * inv
                    cols[s][i] = jnp.where(sub == j, row, cols[s][i] - col * row)
        for s in range(count):
            out[s].append(jnp.where(lane < base + SUB, scaled[s], 0.0))
            rows = [spread_row(here[s], j) for j in range(SUB)]
            for r in range(p + 1, size // SUB):
                tile = tiles[s][r]
                terms = [spread_lane(tile, base + j) * rows[j] for j in range(SUB)]
                while len(terms) > 1:
                    terms = [a + b for a, b in zip(terms[::2], terms[1::2])]
                tiles[s][r] = jnp.where(inside, 0.0, tile) - terms[0]
    return [jnp.concatenate(o, axis=0) for o in out]


def fit_kernel(gnorm_ref, state_ref, near_ref, out_ref, kept_ref, f_ref, hi_ref, mid_ref, low_ref):
    subs, ranks, steps = state_ref.shape
    near = near_ref.shape[1]
    nquad = ranks * (ranks + 1) // 2
    nself = ranks + nquad + 1
    nf = nself + near
    blocks = nf // LANES
    head = blocks * LANES
    rest = -(-(nf - head) // SUB) * SUB
    tall = head + ranks + rest
    gnorm = gnorm_ref[0:1, 0:1]
    kept_ref[...] = state_ref[...]
    keep = (lax.broadcasted_iota(jnp.int32, (1, steps), 1) < steps - 1).astype(jnp.float32)
    last = nf - head
    for s in range(subs):
        state = state_ref[s]
        past = state * keep
        f_ref[s, 0:ranks, :] = past
        at = ranks
        for first in range(ranks):
            f_ref[s, at : at + ranks - first, :] = past[first : first + 1] * state[first:]
            at += ranks - first
        f_ref[s, at : at + 1, :] = keep
        there = near_ref[s] * keep
        f_ref[s, nself:head, :] = there[0 : head - nself]
        f_ref[s, head : head + ranks, :] = pltpu.roll(state, steps - 1, 1)
        f_ref[s, tall - rest : tall, :] = jnp.zeros((rest, steps), jnp.float32)
        f_ref[s, tall - rest : tall - rest + last, :] = there[head - nself :]
        hi, mid, low = split3(f_ref[s])
        hi_ref[s] = hi
        mid_ref[s] = mid
        low_ref[s] = low

    def parts(s, first, size):
        return [r[s, first : first + size, :] for r in (hi_ref, mid_ref, low_ref)]

    linear = beta_linear * gnorm * steps
    square = beta_quad * gnorm * gnorm * steps

    def ridge(first, size, lanes):
        row = lax.broadcasted_iota(jnp.int32, (size, lanes), 0)
        col = lax.broadcasted_iota(jnp.int32, (size, lanes), 1)
        at = row + first
        level = jnp.where((at < ranks) | (at >= nself - 1), linear, square)
        level = jnp.where(at < nf, level, 1.0)
        return jnp.where(row == col, level, 0.0)

    def gram(s, first, rows, at, lanes):
        return dot_nt(as_left(parts(s, first, rows)), as_right(parts(s, at, lanes)))

    g = []
    for s in range(subs):
        cols = []
        for j in range(blocks):
            at = j * LANES
            top = gram(s, at, LANES, at, LANES) + ridge(at, LANES, LANES)
            low = gram(s, at + LANES, tall - at - LANES, at, LANES)
            cols.append([top, low])
        right = gram(s, head, ranks, tall - rest, rest)
        tip = gram(s, tall - rest, rest, tall - rest, rest) + ridge(head, rest, rest)
        cols.append([tip, right])
        g.append(cols)
    roots = [[None] * (blocks + 1) for s in range(subs)]
    sides = [[None] * blocks for s in range(subs)]
    for k in range(blocks):
        done = whiten([g[s][k][0] for s in range(subs)])
        for s in range(subs):
            root = split3(done[s])
            roots[s][k] = root
            side = split3(dot_nt(as_left(split3(g[s][k][1])), as_right(root)))
            sides[s][k] = side
            left = as_left(side)
            right = as_right(side)
            rows = left.shape[0]
            for j in range(k + 1, blocks):
                at = (j - k - 1) * LANES
                both = right[at : at + LANES]
                g[s][j][0] = g[s][j][0] - dot_nt(left[at : at + LANES], both)
                g[s][j][1] = g[s][j][1] - dot_nt(left[at + LANES :], both)
            both = right[rows - rest :]
            g[s][blocks][0] = g[s][blocks][0] - dot_nt(left[rows - rest :], both)
            g[s][blocks][1] = g[s][blocks][1] - dot_nt(left[rows - rest - ranks : rows - rest], both)
    tips = []
    for s in range(subs):
        tip = g[s][blocks][0]
        tips.append(jnp.concatenate([tip, jnp.zeros((rest, LANES - rest), jnp.float32)], axis=1))
    tips = whiten(tips)
    for s in range(subs):
        root = split3(tips[s])
        wide = jnp.concatenate([g[s][blocks][1], jnp.zeros((ranks, LANES - rest), jnp.float32)], axis=1)
        known = dot_nt(as_left(split3(wide)), as_right([jnp.concatenate([p, jnp.zeros((LANES - rest, LANES), p.dtype)], axis=0) for p in root]))
        tail = dot_nn(as_left(split3(known)), as_right([jnp.concatenate([p, jnp.zeros((LANES - rest, LANES), p.dtype)], axis=0) for p in root], 0))
        answer = [None] * (blocks + 1)
        answer[blocks] = tail
        for k in range(blocks - 1, -1, -1):
            hi, mid, low = sides[s][k]
            rows = hi.shape[0]
            value = (hi.astype(jnp.float32) + mid.astype(jnp.float32)) + low.astype(jnp.float32)
            total = value[rows - rest - ranks : rows - rest]
            for j in range(k + 1, blocks):
                at = (j - k - 1) * LANES
                total = total - dot_nn(as_left(split3(answer[j])), as_right([p[at : at + LANES] for p in sides[s][k]], 0))
            pads = [jnp.concatenate([p[rows - rest :], jnp.zeros((LANES - rest, LANES), p.dtype)], axis=0) for p in sides[s][k]]
            total = total - dot_nn(as_left(split3(tail)), as_right(pads, 0))
            answer[k] = dot_nn(as_left(split3(total)), as_right(roots[s][k], 0))
        whole = jnp.concatenate(answer, axis=1)
        out_ref[s] = jnp.concatenate(
            [whole[:, nself - 1 : nself], whole[:, 0:ranks], whole[:, nself:nf], whole[:, ranks : nself - 1]], axis=1
        )


def fit(gnorm, states, near):
    subs, ranks, steps = states.shape
    nf = 1 + ranks + near.shape[1] + ranks * (ranks + 1) // 2
    head = nf // LANES * LANES
    rest = -(-(nf - head) // SUB) * SUB
    tall = head + ranks + rest
    vmem = pl.BlockSpec(memory_space=pltpu.VMEM)
    return pl.pallas_call(
        fit_kernel,
        out_shape=(
            jax.ShapeDtypeStruct((subs, ranks, nf), jnp.float32),
            jax.ShapeDtypeStruct(states.shape, jnp.float32),
        ),
        in_specs=[vmem, vmem, vmem],
        out_specs=(vmem, vmem),
        scratch_shapes=[
            pltpu.VMEM((subs, tall, steps), jnp.float32),
            pltpu.VMEM((subs, tall, steps), jnp.bfloat16),
            pltpu.VMEM((subs, tall, steps), jnp.bfloat16),
            pltpu.VMEM((subs, tall, steps), jnp.bfloat16),
        ],
        compiler_params=pltpu.CompilerParams(vmem_limit_bytes=40 * 2**20),
        name="fit",
    )(gnorm, states, near)


def share_kernel(sizes, counts_ref, links_ref, proj_ref, slotsq_ref, near_ref, state_ref, gnorm_ref,
                 stat_ref, half_ref, row_ref, col_ref, cell_ref, row_sems, col_sems, halo_sems):
    nx, ny = sizes
    subs, nvar, ranks, steps = proj_ref.shape
    slots = slotsq_ref.shape[2]
    nbrs = links_ref.shape[1]
    x, y = lax.axis_index("gx"), lax.axis_index("gy")
    barrier = pltpu.get_barrier_semaphore()
    sides = [(dx, dy) for dx in (-1, 0, 1) for dy in (-1, 0, 1) if dx or dy]

    def at(dx, dy):
        return (lax.rem(x + dx + nx, nx), lax.rem(y + dy + ny, ny))

    greeted = [at(d, 0) for d in range(1, nx)] + [at(0, d) for d in range(1, ny)]
    greeted += [at(dx, dy) for dx, dy in sides if dx and dy]
    for other in greeted:
        pl.semaphore_signal(barrier, inc=1, device_id=other, device_id_type=pl.DeviceIdType.MESH)

    pairs = [(v, w) for v in range(nvar) for w in range(v, nvar)]
    lane = lax.broadcasted_iota(jnp.int32, (1, LANES), 1)
    stat_ref[...] = jnp.zeros(stat_ref.shape, jnp.float32)
    squares = jnp.zeros((nvar, LANES), jnp.float32)
    nodes = 0
    for s in range(subs):
        nodes = nodes + counts_ref[s]
        for p in range(0, slots, LANES):
            squares += jnp.where(lane + p < counts_ref[s], slotsq_ref[s, :, p : p + LANES], 0.0)
    stat_ref[0:nvar, :] = squares
    for i, (v, w) in enumerate(pairs):
        total = jnp.zeros((ranks, LANES), jnp.float32)
        for s in range(subs):
            for k in range(0, steps, LANES):
                total += proj_ref[s, v, :, k : k + LANES] * proj_ref[s, w, :, k : k + LANES]
        stat_ref[nvar + i : nvar + i + 1, :] = jnp.sum(total, axis=0, keepdims=True)
    last = nvar + len(pairs)
    stat_ref[last : last + 1, :] = jnp.where(lane == 0, nodes.astype(jnp.float32), 0.0)

    pl.semaphore_wait(barrier, len(greeted))

    def gather(src, slots_ref, sems, me, count, step):
        slots_ref[me] = src[...]
        copies = []
        for d in range(1, count):
            copies.append(
                pltpu.make_async_remote_copy(
                    src_ref=src,
                    dst_ref=slots_ref.at[me],
                    send_sem=sems.at[0, d],
                    recv_sem=sems.at[1, d],
                    device_id=step(d),
                    device_id_type=pl.DeviceIdType.MESH,
                )
            )
            copies[-1].start()
        for copy in copies:
            copy.wait_recv()
        total = slots_ref[0]
        for d in range(1, count):
            total = total + slots_ref[d]
        return total, copies

    half, sent = gather(stat_ref, row_ref, row_sems, x, nx, lambda d: at(d, 0))
    half_ref[...] = half
    total, more = gather(half_ref, col_ref, col_sems, y, ny, lambda d: at(0, d))
    sent += more
    total = jnp.broadcast_to(jnp.sum(total, axis=1, keepdims=True), total.shape)
    nodes = total[last : last + 1, :]
    scale = [jnp.sqrt(total[v : v + 1, :] / (nodes * steps) + 1e-06) for v in range(nvar)]
    gnorm = jnp.zeros((1, LANES), jnp.float32)
    for i, (v, w) in enumerate(pairs):
        gnorm += (1.0 if v == w else 2.0) * total[nvar + i : nvar + i + 1, :] / (scale[v] * scale[w])
    gnorm = gnorm / (nx * ny * subs * ranks * steps)
    gnorm_ref[...] = jnp.broadcast_to(gnorm, gnorm_ref.shape)
    inverse = [1.0 / part[:, 0:1] for part in scale]
    wide = subs + 2
    for s in range(subs):
        state = proj_ref[s, 0] * inverse[0]
        for v in range(1, nvar):
            state = state + proj_ref[s, v] * inverse[v]
        state_ref[s] = state
        cell_ref[wide + 1 + s] = state
    for i, (dx, dy) in enumerate(sides):
        first, size = (0, subs) if dy == 0 else ((subs - 1, 1) if dy > 0 else (0, 1))
        into = (1 - dx) * wide + (1 if dy == 0 else (0 if dy > 0 else subs + 1))
        copy = pltpu.make_async_remote_copy(
            src_ref=cell_ref.at[pl.ds(wide + 1 + first, size)],
            dst_ref=cell_ref.at[pl.ds(into, size)],
            send_sem=halo_sems.at[0, i],
            recv_sem=halo_sems.at[1, i],
            device_id=at(dx, dy),
            device_id_type=pl.DeviceIdType.MESH,
        )
        copy.start()
        sent.append(copy)
    for i, (dx, dy) in enumerate(sides):
        sent[len(sent) - len(sides) + i].wait_recv()
    for copy in sent:
        copy.wait_send()
    columns = ny * subs
    for s in range(subs):
        for b in range(nbrs):
            link = links_ref[s, b]
            row = link // columns
            cell = (row - x + 1) * wide + link - row * columns - y * subs + 1
            cell = jnp.clip(cell, 0, 3 * wide - 1)
            near_ref[s, b * ranks : b * ranks + ranks, :] = cell_ref[cell]


def share(counts, links, proj, slotsq):
    nx, ny = lax.axis_size("gx"), lax.axis_size("gy")
    subs, nvar, ranks, steps = proj.shape
    rows = -(-(nvar + nvar * (nvar + 1) // 2 + 1) // SUB) * SUB
    smem = pl.BlockSpec(memory_space=pltpu.SMEM)
    vmem = pl.BlockSpec(memory_space=pltpu.VMEM)

    def kernel(*refs):
        share_kernel((nx, ny), *refs)

    return pl.pallas_call(
        kernel,
        out_shape=(
            jax.ShapeDtypeStruct((subs, links.shape[1] * ranks, steps), jnp.float32),
            jax.ShapeDtypeStruct((subs, ranks, steps), jnp.float32),
            jax.ShapeDtypeStruct((SUB, LANES), jnp.float32),
        ),
        in_specs=[smem, smem, vmem, vmem],
        out_specs=(vmem, vmem, vmem),
        scratch_shapes=[
            pltpu.VMEM((rows, LANES), jnp.float32),
            pltpu.VMEM((rows, LANES), jnp.float32),
            pltpu.VMEM((nx, rows, LANES), jnp.float32),
            pltpu.VMEM((ny, rows, LANES), jnp.float32),
            pltpu.VMEM((3 * (subs + 2), ranks, steps), jnp.float32),
            pltpu.SemaphoreType.DMA((2, nx)),
            pltpu.SemaphoreType.DMA((2, ny)),
            pltpu.SemaphoreType.DMA((2, 8)),
        ],
        compiler_params=pltpu.CompilerParams(collective_id=0, has_side_effects=True),
        name="share",
    )(counts, links, proj, slotsq)


def body(snapshots, basis, node_counts, adjacency):
    values = snapshots[0]
    modes = basis[0]
    counts = node_counts[0]
    slots = values.shape[2]
    live = jnp.arange(slots, dtype=jnp.int32)[None, :] < counts[:, None]
    masked = modes * live.astype(jnp.bfloat16)[:, None, None, :]
    proj = jnp.einsum("svrp,svpk->svrk", masked, values, preferred_element_type=jnp.float32)
    slotsq = jnp.einsum("svpk,svpk->svp", values, values, preferred_element_type=jnp.float32)
    near, states, gnorm = share(counts, adjacency[0], proj, slotsq)
    operator, states = fit(gnorm, states, near)
    return (operator.swapaxes(1, 2)[None], states[None])


def solution(mesh):
    in_specs = (
        P("gx", "gy", None, None, None),
        P("gx", "gy", None, None, None),
        P("gx", "gy"),
        P("gx", "gy", None),
    )
    out_specs = (P("gx", "gy", None, None), P("gx", "gy", None, None))
    return jax.shard_map(body, mesh=mesh, in_specs=in_specs, out_specs=out_specs, check_vma=False)
```

```python
import jax
import jax.numpy as jnp
from jax import lax
from jax.experimental import pallas as pl
from jax.experimental.pallas import tpu as pltpu
from jax.sharding import PartitionSpec as P

beta_linear = 0.5
beta_quad = 0.5
LANES = 128
SUB = 8
STEP = 16
join = 2


def split3(a):
    hi = a.astype(jnp.bfloat16)
    left = a - hi.astype(jnp.float32)
    mid = left.astype(jnp.bfloat16)
    low = (left - mid.astype(jnp.float32)).astype(jnp.bfloat16)
    return hi, mid, low


def as_left(parts):
    hi, mid, low = parts
    return jnp.concatenate([hi, mid, hi, mid, hi, low], axis=1)


def as_right(parts, axis=1):
    hi, mid, low = parts
    return jnp.concatenate([hi, mid, mid, hi, low, hi], axis=axis)


def dot_nt(a, b):
    return lax.dot_general(a, b, (((1,), (1,)), ((), ())), preferred_element_type=jnp.float32)


def dot_nn(a, b):
    return jnp.dot(a, b, preferred_element_type=jnp.float32)


def pick(tile, index):
    rows = [
        jnp.take_along_axis(tile[r : r + SUB], index, axis=1, mode="promise_in_bounds")
        for r in range(0, tile.shape[0], SUB)
    ]
    return rows[0] if len(rows) == 1 else jnp.concatenate(rows, axis=0)


def whiten(block, wide):
    size = block.shape[0]
    lane8 = lax.broadcasted_iota(jnp.int32, (SUB, LANES), 1)
    half = lane8 - lane8 % wide
    lane = lax.broadcasted_iota(jnp.int32, (1, LANES), 1) % wide
    done = []
    rest = block
    for base in range(0, size, STEP):
        row = lax.broadcasted_iota(jnp.int32, (STEP, LANES), 0)
        inside = (lane >= base) & (lane < base + STEP)
        here = rest[0:STEP]
        rest = rest[STEP:]
        cols = jnp.stack([pick(here, half + (base + j)) for j in range(STEP)])
        side = [pick(rest, half + (base + j)) for j in range(STEP)] if rest.shape[0] else None
        here = jnp.where(inside, (lane - base == row).astype(jnp.float32), here)
        scaled = jnp.zeros((STEP, LANES), jnp.float32)
        for j in range(STEP):
            col = cols[0]
            inv = 1.0 / col[j : j + 1]
            now = here[j : j + 1]
            scaled = jnp.where(row == j, now * lax.rsqrt(col[j : j + 1]), scaled)
            now = now * inv
            here = jnp.where(row == j, now, here - col * now)
            if j + 1 < STEP:
                cols = cols[1:]
                top = cols[:, j : j + 1, :] * inv
                cols = jnp.where(row == j, top, cols - col * top)
        done.append(jnp.where(lane < base + STEP, scaled, 0.0))
        if rest.shape[0]:
            terms = [side[j] * here[j : j + 1] for j in range(STEP)]
            while len(terms) > 1:
                terms = [a + b for a, b in zip(terms[::2], terms[1::2])]
            rest = jnp.where(inside, 0.0, rest) - terms[0]
    return done[0] if len(done) == 1 else jnp.concatenate(done, axis=0)


def shape_of(subs, ranks, near):
    wide = LANES // subs
    nself = 1 + ranks + ranks * (ranks + 1) // 2
    nf = nself + near
    full = nf // wide
    early = nself // wide
    rest = -(-(nf - full * wide) // STEP) * STEP
    return wide, nself, nf, full, early, rest, full * wide + ranks + rest


def fit_body(gnorm, state_of, near_of, out_ref, f_ref, part_refs, subs, ranks, near, steps):
    wide, nself, nf, full, early, rest, tall = shape_of(subs, ranks, near)
    head = early * wide
    late = head + ranks
    keep = (lax.broadcasted_iota(jnp.int32, (1, steps), 1) < steps - 1).astype(jnp.float32)

    def place(s, first, size):
        for ref, part in zip(part_refs, split3(f_ref[s, first : first + size, :])):
            ref[s, first : first + size, :] = part

    tailing = []
    for s in range(subs):
        state = state_of(s)
        past = state * keep
        f_ref[s, 0:ranks, :] = past
        at = ranks
        for first in range(ranks):
            rows = past[first : first + 1] * state[first:]
            cut = max(0, min(ranks - first, head - at))
            if cut:
                f_ref[s, at : at + cut, :] = rows[:cut]
            if cut < ranks - first:
                tailing_at = at + cut - head + late
                f_ref[s, tailing_at : tailing_at + ranks - first - cut, :] = rows[cut:]
            at += ranks - first
        f_ref[s, head:late, :] = pltpu.roll(state, steps - 1, 1)
        f_ref[s, late + nself - 1 - head : late + nself - head, :] = keep
        place(s, 0, late)

    linear = beta_linear * gnorm * steps
    square = beta_quad * gnorm * gnorm * steps

    def ridge(first, size):
        row = lax.broadcasted_iota(jnp.int32, (size, LANES), 0)
        col = lax.broadcasted_iota(jnp.int32, (size, LANES), 1) % wide
        at = row + first
        level = jnp.where((at < ranks) | (at >= nself - 1), linear, square)
        level = jnp.where(at < nf, level, 1.0)
        return jnp.where(row == col, level, 0.0)

    def rows_at(j):
        return j * wide if j < early else late + (j - early) * wide

    def size_of(j):
        return wide if j < full else rest

    def gram(first, size, j):
        at, span = rows_at(j), size_of(j)
        total = None
        for s in range(subs):
            left = as_left([r[s, first : first + size, :] for r in part_refs])
            parts = []
            for r in part_refs:
                pieces = [r[s, at : at + span, :]]
                if s * wide:
                    pieces.insert(0, jnp.zeros((s * wide, steps), r.dtype))
                if LANES - s * wide - span:
                    pieces.append(jnp.zeros((LANES - s * wide - span, steps), r.dtype))
                parts.append(jnp.concatenate(pieces, axis=0))
            one = dot_nt(left, as_right(parts))
            total = one if total is None else total + one
        return total

    lanes = lax.broadcasted_iota(jnp.int32, (1, LANES), 1) // wide

    def pair(block):
        if block.shape[0] < wide:
            block = jnp.concatenate([block, jnp.zeros((wide - block.shape[0], LANES), block.dtype)], axis=0)
        return jnp.concatenate([jnp.where(lanes == s, block, 0.0) for s in range(subs)], axis=0)

    roots, tops, sides, lefts, boths = {}, {}, {}, {}, {}

    def extent(j, part):
        if part == 1:
            return (max(late, rows_at(j) + wide), tall)
        return (rows_at(j) + wide, late) if j < early else (head, late)

    def cut(table, k, first, last):
        part = int(first >= late)
        start = extent(k, part)[0]
        return table[k, part][first - start : last - start]

    def both(k, j):
        if (k, j) not in boths:
            block = cut(sides, k, rows_at(j), rows_at(j) + size_of(j))
            boths[k, j] = as_right(split3(pair(block)))
        return boths[k, j]

    def less(value, j, first, last, before):
        for k in before:
            value = value - dot_nt(cut(lefts, k, first, last), both(k, j))
        return value

    def top_of(j, before):
        if j not in tops:
            tops[j] = gram(rows_at(j), size_of(j), j) + ridge(j * wide, size_of(j))
        first = rows_at(j)
        tops[j] = less(tops[j], j, first, first + size_of(j), before)

    lows = {}

    def low_of(j, part, before):
        first, last = extent(j, part)
        if last > first:
            if (j, part) not in lows:
                lows[j, part] = gram(first, last - first, j)
            lows[j, part] = less(lows[j, part], j, first, last, before)

    def settle(j, part):
        if (j, part) in lows:
            side = dot_nt(as_left(split3(lows[j, part])), as_right(roots[j]))
            sides[j, part] = side
            lefts[j, part] = as_left(split3(side))

    def bring():
        for s in range(subs):
            there = near_of(s) * keep
            at = late + nself - head
            f_ref[s, at : at + near, :] = there
            f_ref[s, at + near : tall, :] = jnp.zeros((tall - at - near, steps), jnp.float32)
            place(s, late, tall - late)

    top_of(0, ())
    low_of(0, 0, ())
    for k in range(full + 1):
        if k == join:
            bring()
            for j in range(join):
                low_of(j, 1, range(j))
                settle(j, 1)
        roots[k] = split3(pair(whiten(tops[k], wide)))
        after = k + 1 if k < full else None
        if k >= join:
            low_of(k, 1, range(k))
        if after is not None and (after < early or k >= join):
            top_of(after, range(k))
            low_of(after, 0, range(k))
        settle(k, 0)
        if k >= join:
            settle(k, 1)
        if after is not None:
            if after < early or k >= join:
                top_of(after, (k,))
                low_of(after, 0, (k,))
    answer = [None] * (full + 1)
    scaled = {}
    for key, left in lefts.items():
        scaled[key] = dot_nn(left, as_right(roots[key[0]], 0))
    for k in range(full, -1, -1):
        total = cut(scaled, k, head, late)
        for j in range(full, k, -1):
            block = cut(scaled, k, rows_at(j), rows_at(j) + size_of(j))
            total = total - dot_nn(as_left(split3(answer[j])), as_right(split3(pair(block)), 0))
        answer[k] = total
    for s in range(subs):
        def lanes_of(first, last):
            out = []
            while first < last:
                k = first // wide
                end = min(last, (k + 1) * wide)
                out.append(answer[k][:, s * wide + first - k * wide : s * wide + end - k * wide])
                first = end
            return out
        order = lanes_of(nself - 1, nself) + lanes_of(0, ranks) + lanes_of(nself, nf) + lanes_of(ranks, nself - 1)
        out_ref[s] = jnp.concatenate(order, axis=1)


def fit_kernel(gnorm_ref, state_ref, near_ref, out_ref, kept_ref, f_ref, *part_refs):
    subs, ranks, steps = state_ref.shape
    kept_ref[...] = state_ref[...]
    fit_body(gnorm_ref[0:1, 0:1], lambda s: state_ref[s], lambda s: near_ref[s], out_ref, f_ref, part_refs,
             subs, ranks, near_ref.shape[1], steps)


def fit(gnorm, states, near):
    subs, ranks, steps = states.shape
    wide, nself, nf, full, early, rest, tall = shape_of(subs, ranks, near.shape[1])
    vmem = pl.BlockSpec(memory_space=pltpu.VMEM)
    return pl.pallas_call(
        fit_kernel,
        out_shape=(
            jax.ShapeDtypeStruct((subs, ranks, nf), jnp.float32),
            jax.ShapeDtypeStruct(states.shape, jnp.float32),
        ),
        in_specs=[vmem, vmem, vmem],
        out_specs=(vmem, vmem),
        scratch_shapes=[pltpu.VMEM((subs, tall, steps), jnp.float32)]
        + [pltpu.VMEM((subs, tall, steps), jnp.bfloat16)] * 3,
        compiler_params=pltpu.CompilerParams(vmem_limit_bytes=40 * 2**20),
        name="fit",
    )(gnorm, states, near)


CHUNKS = 4
ROWS = 64


def everyone(sizes):
    nx, ny = sizes
    x, y = lax.axis_index("gx"), lax.axis_index("gy")

    def at(dx, dy):
        return (lax.rem(x + dx + nx, nx), lax.rem(y + dy + ny, ny))

    others = [at(dx, dy) for dx in range(nx) for dy in range(ny) if dx or dy]
    return x, y, at, others


def gather_kernel(sizes, subs, nvar, counts_ref, snaps_ref, basis_ref, stage):
    nx, ny = sizes
    snap_ref, base_ref, proj_ref, square_ref, row_ref, all_ref, snap_sems, base_sems, row_sems = stage
    count, slots, steps = snap_ref.shape
    ranks = base_ref.shape[1]
    part = slots // CHUNKS
    x, y, at, others = everyone(sizes)

    def piece(i, c):
        span = pl.ds(c * part, part)
        return pltpu.make_async_copy(snaps_ref.at[i, span], snap_ref.at[i, span], snap_sems.at[i, c])

    def modes(i):
        return pltpu.make_async_copy(basis_ref.at[i], base_ref.at[i], base_sems.at[i])

    for i in range(count):
        modes(i).start()
        for c in range(CHUNKS):
            piece(i, c).start()
    barrier = pltpu.get_barrier_semaphore()
    for other in others:
        pl.semaphore_signal(barrier, inc=1, device_id=other, device_id_type=pl.DeviceIdType.MESH)

    def project(i, carry):
        live = counts_ref[i // nvar]
        modes(i).wait()
        lane = lax.broadcasted_iota(jnp.int32, (1, slots), 1)
        mask = jnp.where(lane < live, 1.0, 0.0).astype(jnp.bfloat16)
        masked = base_ref[i] * mask
        total = jnp.zeros((ranks, steps), jnp.float32)
        squares = jnp.zeros((SUB, LANES), jnp.float32)
        for c in range(CHUNKS):
            piece(i, c).wait()
            total = total + jnp.dot(
                masked[:, c * part : (c + 1) * part],
                snap_ref[i, c * part : (c + 1) * part, :],
                preferred_element_type=jnp.float32,
            )
            for first in range(c * part, (c + 1) * part, ROWS):
                value = snap_ref[i, first : first + ROWS, :].astype(jnp.float32)
                value = value * value
                value = sum(value[:, k : k + LANES] for k in range(0, steps, LANES))
                node = lax.broadcasted_iota(jnp.int32, (ROWS, LANES), 0) + first
                value = jnp.where(node < live, value, 0.0)
                squares = squares + jnp.sum(value.reshape(ROWS // SUB, SUB, LANES), axis=0)
        proj_ref[i] = total
        square_ref[i] = squares
        return carry

    lax.fori_loop(0, count, project, 0)

    pairs = [(v, w) for v in range(nvar) for w in range(v, nvar)]
    rows = []
    for v in range(nvar):
        rows.append(sum(square_ref[s * nvar + v] for s in range(subs)))
    for v, w in pairs:
        both = sum(proj_ref[s * nvar + v] * proj_ref[s * nvar + w] for s in range(subs))
        both = sum(both[:, k : k + LANES] for k in range(0, steps, LANES))
        rows.append(jnp.sum(both.reshape(ranks // SUB, SUB, LANES), axis=0))
    nodes = counts_ref[0]
    for s in range(1, subs):
        nodes = nodes + counts_ref[s]
    tall = -(-len(rows) // SUB) * SUB
    index = lax.broadcasted_iota(jnp.int32, (tall, LANES), 0)
    lane = lax.broadcasted_iota(jnp.int32, (tall, LANES), 1)
    table = jnp.zeros((tall, LANES), jnp.float32)
    for i, row in enumerate(rows):
        table = jnp.where(index == i, jnp.sum(row, axis=0, keepdims=True), table)
    table = jnp.broadcast_to(jnp.sum(table, axis=1, keepdims=True), table.shape)
    table = jnp.sum(jnp.where(index == lane, table, 0.0), axis=0, keepdims=True)
    row = jnp.where(lane[0:1] == len(rows), nodes.astype(jnp.float32), table)
    me = x * ny + y
    row_ref[0] = row
    all_ref[me] = row
    pl.semaphore_wait(barrier, len(others))
    sent = []
    for d, other in enumerate(others):
        copy = pltpu.make_async_remote_copy(
            src_ref=row_ref.at[0],
            dst_ref=all_ref.at[me],
            send_sem=row_sems.at[0, d],
            recv_sem=row_sems.at[1, d],
            device_id=other,
            device_id_type=pl.DeviceIdType.MESH,
        )
        copy.start()
        sent.append(copy)
    for copy in sent:
        copy.wait_recv()
    total = jnp.sum(all_ref[...], axis=0)
    stat = [jnp.broadcast_to(total[:, i : i + 1], (1, LANES)) for i in range(len(rows) + 1)]
    nodes = stat[len(rows)]
    scale = [jnp.sqrt(stat[v] / (nodes * steps) + 1e-06) for v in range(nvar)]
    inverse = [1.0 / part for part in scale]
    gnorm = jnp.zeros((1, LANES), jnp.float32)
    for i, (v, w) in enumerate(pairs):
        gnorm += (1.0 if v == w else 2.0) * stat[nvar + i] * (inverse[v] * inverse[w])
    gnorm = gnorm / (nx * ny * subs * ranks * steps)
    states = []
    for s in range(subs):
        state = proj_ref[s * nvar] * inverse[0][:, 0:1]
        for v in range(1, nvar):
            state = state + proj_ref[s * nvar + v] * inverse[v][:, 0:1]
        states.append(state)
    return gnorm, states, sent


class Halo:
    def __init__(self, sizes, subs, cell_ref, sems):
        nx, ny = sizes
        x, y, at, others = everyone(sizes)
        wide = subs + 2
        self.x, self.y, self.ny, self.subs, self.wide, self.cells = x, y, ny, subs, wide, cell_ref
        self.copies = []
        sides = [(dx, dy) for dx in (-1, 0, 1) for dy in (-1, 0, 1) if dx or dy]
        for i, (dx, dy) in enumerate(sides):
            first, size = (0, subs) if dy == 0 else ((subs - 1, 1) if dy > 0 else (0, 1))
            into = (1 - dx) * wide + (1 if dy == 0 else (0 if dy > 0 else subs + 1))
            copy = pltpu.make_async_remote_copy(
                src_ref=cell_ref.at[pl.ds(wide + 1 + first, size)],
                dst_ref=cell_ref.at[pl.ds(into, size)],
                send_sem=sems.at[0, i],
                recv_sem=sems.at[1, i],
                device_id=at(dx, dy),
                device_id_type=pl.DeviceIdType.MESH,
            )
            sends = (x + dx >= 0) & (x + dx < nx) & (y + dy >= 0) & (y + dy < ny)
            takes = (x - dx >= 0) & (x - dx < nx) & (y - dy >= 0) & (y - dy < ny)
            self.copies.append((copy, sends, takes))

    def start(self, states):
        for s, state in enumerate(states):
            self.cells[self.wide + 1 + s] = state
        for copy, sends, takes in self.copies:
            pl.when(sends)(copy.start)

    def arrive(self):
        for copy, sends, takes in self.copies:
            pl.when(takes)(copy.wait_recv)

    def finish(self):
        for copy, sends, takes in self.copies:
            pl.when(sends)(copy.wait_send)

    def near(self, links_ref, s):
        columns = self.ny * self.subs
        found = []
        for b in range(links_ref.shape[1]):
            link = links_ref[s, b]
            row = link // columns
            cell = (row - self.x + 1) * self.wide + link - row * columns - self.y * self.subs + 1
            found.append(self.cells[jnp.clip(cell, 0, 3 * self.wide - 1)])
        return found


def share_kernel(sizes, subs, nvar, counts_ref, links_ref, snaps_ref, basis_ref, near_ref, state_ref, gnorm_ref, cell_ref, halo_sems, *stage):
    ranks = state_ref.shape[1]
    gnorm, states, sent = gather_kernel(sizes, subs, nvar, counts_ref, snaps_ref, basis_ref, stage)
    halo = Halo(sizes, subs, cell_ref, halo_sems)
    halo.start(states)
    gnorm_ref[...] = jnp.broadcast_to(gnorm, gnorm_ref.shape)
    for s in range(subs):
        state_ref[s] = states[s]
    halo.arrive()
    for s in range(subs):
        for b, found in enumerate(halo.near(links_ref, s)):
            near_ref[s, b * ranks : b * ranks + ranks, :] = found
    for copy in sent:
        copy.wait_send()
    halo.finish()


def stage_shapes(devices, count, slots, ranks, steps):
    return [
        pltpu.VMEM((count, slots, steps), jnp.bfloat16),
        pltpu.VMEM((count, ranks, slots), jnp.bfloat16),
        pltpu.VMEM((count, ranks, steps), jnp.float32),
        pltpu.VMEM((count, SUB, LANES), jnp.float32),
        pltpu.VMEM((1, 1, LANES), jnp.float32),
        pltpu.VMEM((devices, 1, LANES), jnp.float32),
        pltpu.SemaphoreType.DMA((count, CHUNKS)),
        pltpu.SemaphoreType.DMA((count,)),
        pltpu.SemaphoreType.DMA((2, devices - 1)),
    ]


def share(counts, links, snaps, basis):
    nx, ny = lax.axis_size("gx"), lax.axis_size("gy")
    subs, nvar, ranks, slots = basis.shape
    steps = snaps.shape[3]
    smem = pl.BlockSpec(memory_space=pltpu.SMEM)
    vmem = pl.BlockSpec(memory_space=pltpu.VMEM)
    hbm = pl.BlockSpec(memory_space=pltpu.HBM)

    def kernel(*refs):
        share_kernel((nx, ny), subs, nvar, *refs)

    return pl.pallas_call(
        kernel,
        out_shape=(
            jax.ShapeDtypeStruct((subs, links.shape[1] * ranks, steps), jnp.float32),
            jax.ShapeDtypeStruct((subs, ranks, steps), jnp.float32),
            jax.ShapeDtypeStruct((SUB, LANES), jnp.float32),
        ),
        in_specs=[smem, smem, hbm, hbm],
        out_specs=(vmem, vmem, vmem),
        scratch_shapes=[
            pltpu.VMEM((3 * (subs + 2), ranks, steps), jnp.float32),
            pltpu.SemaphoreType.DMA((2, 8)),
        ]
        + stage_shapes(nx * ny, subs * nvar, slots, ranks, steps),
        compiler_params=pltpu.CompilerParams(collective_id=0, has_side_effects=True, vmem_limit_bytes=60 * 2**20),
        name="share",
    )(counts, links, snaps.reshape(subs * nvar, slots, steps), basis.reshape(subs * nvar, ranks, slots))


def body(snapshots, basis, node_counts, adjacency):
    near, states, gnorm = share(node_counts[0], adjacency[0], snapshots[0], basis[0])
    operator, states = fit(gnorm, states, near)
    return (operator.swapaxes(1, 2)[None], states[None])


def solution(mesh):
    in_specs = (
        P("gx", "gy", None, None, None),
        P("gx", "gy", None, None, None),
        P("gx", "gy"),
        P("gx", "gy", None),
    )
    out_specs = (P("gx", "gy", None, None), P("gx", "gy", None, None))
    return jax.shard_map(body, mesh=mesh, in_specs=in_specs, out_specs=out_specs, check_vma=False)
```

```python
import jax
import jax.numpy as jnp
from jax import lax
from jax.experimental import pallas as pl
from jax.experimental.pallas import tpu as pltpu
from jax.sharding import PartitionSpec as P

beta_linear = 0.5
beta_quad = 0.5
LANES = 128
SUB = 8
STEP = 16
join = 2


def split3(a):
    hi = a.astype(jnp.bfloat16)
    left = a - hi.astype(jnp.float32)
    mid = left.astype(jnp.bfloat16)
    low = (left - mid.astype(jnp.float32)).astype(jnp.bfloat16)
    return hi, mid, low


def as_left(parts):
    hi, mid, low = parts
    return jnp.concatenate([hi, mid, hi, mid, hi, low], axis=1)


def as_right(parts, axis=1):
    hi, mid, low = parts
    return jnp.concatenate([hi, mid, mid, hi, low, hi], axis=axis)


def dot_nt(a, b):
    return lax.dot_general(a, b, (((1,), (1,)), ((), ())), preferred_element_type=jnp.float32)


def dot_nn(a, b):
    return jnp.dot(a, b, preferred_element_type=jnp.float32)


ALONG = lax.GatherDimensionNumbers(
    offset_dims=(), collapsed_slice_dims=(1,), start_index_map=(1,), operand_batching_dims=(0,), start_indices_batching_dims=(0,)
)


def pick(tile, index):
    rows = [
        lax.gather(tile[r : r + SUB], index, ALONG, (1, 1), mode=lax.GatherScatterMode.PROMISE_IN_BOUNDS)
        for r in range(0, tile.shape[0], SUB)
    ]
    return rows[0] if len(rows) == 1 else jnp.concatenate(rows, axis=0)


def whiten(block, wide):
    size = block.shape[0]
    lane8 = lax.broadcasted_iota(jnp.int32, (SUB, LANES), 1)
    half = lane8 - lane8 % wide
    lane = lax.broadcasted_iota(jnp.int32, (1, LANES), 1) % wide
    done = []
    rest = block
    for base in range(0, size, STEP):
        row = lax.broadcasted_iota(jnp.int32, (STEP, LANES), 0)
        inside = (lane >= base) & (lane < base + STEP)
        here = rest[0:STEP]
        rest = rest[STEP:]
        index = [(half + (base + j))[:, :, None] for j in range(STEP)]
        cols = jnp.stack([pick(here, index[j]) for j in range(STEP)])
        side = [pick(rest, index[j]) for j in range(STEP)] if rest.shape[0] else None
        here = jnp.where(inside, (lane - base == row).astype(jnp.float32), here)
        scaled = jnp.zeros((STEP, LANES), jnp.float32)
        for j in range(STEP):
            col = cols[0]
            inv = 1.0 / col[j : j + 1]
            now = here[j : j + 1]
            scaled = jnp.where(row == j, now * lax.rsqrt(col[j : j + 1]), scaled)
            now = now * inv
            here = jnp.where(row == j, now, here - col * now)
            if j + 1 < STEP:
                cols = cols[1:]
                top = cols[:, j : j + 1, :] * inv
                cols = jnp.where(row == j, top, cols - col * top)
        done.append(jnp.where(lane < base + STEP, scaled, 0.0))
        if rest.shape[0]:
            terms = [side[j] * here[j : j + 1] for j in range(STEP)]
            while len(terms) > 1:
                terms = [a + b for a, b in zip(terms[::2], terms[1::2])]
            rest = jnp.where(inside, 0.0, rest) - terms[0]
    return done[0] if len(done) == 1 else jnp.concatenate(done, axis=0)


def shape_of(subs, ranks, near):
    wide = LANES // subs
    nself = 1 + ranks + ranks * (ranks + 1) // 2
    nf = nself + near
    full = nf // wide
    early = nself // wide
    rest = -(-(nf - full * wide) // STEP) * STEP
    return wide, nself, nf, full, early, rest, full * wide + ranks + rest


def fit_body(gnorm, state_of, near_of, arrive, out_ref, f_ref, part_refs, subs, ranks, near, steps):
    wide, nself, nf, full, early, rest, tall = shape_of(subs, ranks, near)
    head = early * wide
    late = head + ranks
    keep = (lax.broadcasted_iota(jnp.int32, (1, steps), 1) < steps - 1).astype(jnp.float32)

    def place(s, first, size):
        for ref, part in zip(part_refs, split3(f_ref[s, first : first + size, :])):
            ref[s, first : first + size, :] = part

    tailing = []
    for s in range(subs):
        state = state_of(s)
        past = state * keep
        f_ref[s, 0:ranks, :] = past
        at = ranks
        for first in range(ranks):
            rows = past[first : first + 1] * state[first:]
            cut = max(0, min(ranks - first, head - at))
            if cut:
                f_ref[s, at : at + cut, :] = rows[:cut]
            if cut < ranks - first:
                tailing_at = at + cut - head + late
                f_ref[s, tailing_at : tailing_at + ranks - first - cut, :] = rows[cut:]
            at += ranks - first
        f_ref[s, head:late, :] = pltpu.roll(state, steps - 1, 1)
        f_ref[s, late + nself - 1 - head : late + nself - head, :] = keep
        place(s, 0, late)

    linear = beta_linear * gnorm * steps
    square = beta_quad * gnorm * gnorm * steps

    def ridge(first, size):
        row = lax.broadcasted_iota(jnp.int32, (size, LANES), 0)
        col = lax.broadcasted_iota(jnp.int32, (size, LANES), 1) % wide
        at = row + first
        level = jnp.where((at < ranks) | (at >= nself - 1), linear, square)
        level = jnp.where(at < nf, level, 1.0)
        return jnp.where(row == col, level, 0.0)

    def rows_at(j):
        return j * wide if j < early else late + (j - early) * wide

    def size_of(j):
        return wide if j < full else rest

    def gram(first, size, j):
        at, span = rows_at(j), size_of(j)
        total = None
        for s in range(subs):
            left = as_left([r[s, first : first + size, :] for r in part_refs])
            parts = []
            for r in part_refs:
                pieces = [r[s, at : at + span, :]]
                if s * wide:
                    pieces.insert(0, jnp.zeros((s * wide, steps), r.dtype))
                if LANES - s * wide - span:
                    pieces.append(jnp.zeros((LANES - s * wide - span, steps), r.dtype))
                parts.append(jnp.concatenate(pieces, axis=0))
            one = dot_nt(left, as_right(parts))
            total = one if total is None else total + one
        return total

    lanes = lax.broadcasted_iota(jnp.int32, (1, LANES), 1) // wide

    def pair(block):
        if block.shape[0] < wide:
            block = jnp.concatenate([block, jnp.zeros((wide - block.shape[0], LANES), block.dtype)], axis=0)
        return jnp.concatenate([jnp.where(lanes == s, block, 0.0) for s in range(subs)], axis=0)

    roots, tops, sides, lefts, boths = {}, {}, {}, {}, {}

    def extent(j, part):
        if part == 1:
            return (max(late, rows_at(j) + wide), tall)
        return (rows_at(j) + wide, late) if j < early else (head, late)

    def cut(table, k, first, last):
        part = int(first >= late)
        start = extent(k, part)[0]
        return table[k, part][first - start : last - start]

    def both(k, j):
        if (k, j) not in boths:
            block = cut(sides, k, rows_at(j), rows_at(j) + size_of(j))
            boths[k, j] = as_right(split3(pair(block)))
        return boths[k, j]

    def less(value, j, first, last, before):
        for k in before:
            value = value - dot_nt(cut(lefts, k, first, last), both(k, j))
        return value

    def top_of(j, before):
        if j not in tops:
            tops[j] = gram(rows_at(j), size_of(j), j) + ridge(j * wide, size_of(j))
        first = rows_at(j)
        tops[j] = less(tops[j], j, first, first + size_of(j), before)

    lows = {}

    def low_of(j, part, before):
        first, last = extent(j, part)
        if last > first:
            if (j, part) not in lows:
                lows[j, part] = gram(first, last - first, j)
            lows[j, part] = less(lows[j, part], j, first, last, before)

    def settle(j, part):
        if (j, part) in lows:
            side = dot_nt(as_left(split3(lows[j, part])), as_right(roots[j]))
            sides[j, part] = side
            lefts[j, part] = as_left(split3(side))

    def bring():
        arrive()
        for s in range(subs):
            there = near_of(s) * keep
            at = late + nself - head
            f_ref[s, at : at + near, :] = there
            f_ref[s, at + near : tall, :] = jnp.zeros((tall - at - near, steps), jnp.float32)
            place(s, late, tall - late)

    top_of(0, ())
    low_of(0, 0, ())
    for k in range(full + 1):
        if k == join:
            bring()
            for j in range(join):
                low_of(j, 1, range(j))
                settle(j, 1)
        roots[k] = split3(pair(whiten(tops[k], wide)))
        after = k + 1 if k < full else None
        if k >= join:
            low_of(k, 1, range(k))
        if after is not None and (after < early or k >= join):
            top_of(after, range(k))
            low_of(after, 0, range(k))
        settle(k, 0)
        if k >= join:
            settle(k, 1)
        if after is not None:
            if after < early or k >= join:
                top_of(after, (k,))
                low_of(after, 0, (k,))
    answer = [None] * (full + 1)
    scaled = {}
    for key, left in lefts.items():
        scaled[key] = dot_nn(left, as_right(roots[key[0]], 0))
    for k in range(full, -1, -1):
        total = cut(scaled, k, head, late)
        for j in range(full, k, -1):
            block = cut(scaled, k, rows_at(j), rows_at(j) + size_of(j))
            total = total - dot_nn(as_left(split3(answer[j])), as_right(split3(pair(block)), 0))
        answer[k] = total
    for s in range(subs):
        def lanes_of(first, last):
            out = []
            while first < last:
                k = first // wide
                end = min(last, (k + 1) * wide)
                out.append(answer[k][:, s * wide + first - k * wide : s * wide + end - k * wide])
                first = end
            return out
        order = lanes_of(nself - 1, nself) + lanes_of(0, ranks) + lanes_of(nself, nf) + lanes_of(ranks, nself - 1)
        out_ref[s] = jnp.concatenate(order, axis=1)


CHUNKS = 4
ROWS = 64


def everyone(sizes):
    nx, ny = sizes
    x, y = lax.axis_index("gx"), lax.axis_index("gy")

    def at(dx, dy):
        return (lax.rem(x + dx + nx, nx), lax.rem(y + dy + ny, ny))

    others = [at(dx, dy) for dx in range(nx) for dy in range(ny) if dx or dy]
    return x, y, at, others


def gather_kernel(sizes, subs, nvar, counts_ref, snaps_ref, basis_ref, stage):
    nx, ny = sizes
    snap_ref, base_ref, proj_ref, square_ref, row_ref, all_ref, snap_sems, base_sems, row_sems = stage
    count, slots, steps = snap_ref.shape
    ranks = base_ref.shape[1]
    part = slots // CHUNKS
    x, y, at, others = everyone(sizes)

    def piece(i, c):
        span = pl.ds(c * part, part)
        return pltpu.make_async_copy(snaps_ref.at[i, span], snap_ref.at[i, span], snap_sems.at[i, c])

    def modes(i):
        return pltpu.make_async_copy(basis_ref.at[i], base_ref.at[i], base_sems.at[i])

    for i in range(count):
        modes(i).start()
        for c in range(CHUNKS):
            piece(i, c).start()
    barrier = pltpu.get_barrier_semaphore()
    for other in others:
        pl.semaphore_signal(barrier, inc=1, device_id=other, device_id_type=pl.DeviceIdType.MESH)

    def project(i, carry):
        live = counts_ref[i // nvar]
        modes(i).wait()
        lane = lax.broadcasted_iota(jnp.int32, (1, slots), 1)
        mask = jnp.where(lane < live, 1.0, 0.0).astype(jnp.bfloat16)
        masked = base_ref[i] * mask
        total = jnp.zeros((ranks, steps), jnp.float32)
        squares = jnp.zeros((SUB, LANES), jnp.float32)
        for c in range(CHUNKS):
            piece(i, c).wait()
            total = total + jnp.dot(
                masked[:, c * part : (c + 1) * part],
                snap_ref[i, c * part : (c + 1) * part, :],
                preferred_element_type=jnp.float32,
            )
            for first in range(c * part, (c + 1) * part, ROWS):
                value = snap_ref[i, first : first + ROWS, :].astype(jnp.float32)
                value = value * value
                value = sum(value[:, k : k + LANES] for k in range(0, steps, LANES))
                node = lax.broadcasted_iota(jnp.int32, (ROWS, LANES), 0) + first
                value = jnp.where(node < live, value, 0.0)
                squares = squares + jnp.sum(value.reshape(ROWS // SUB, SUB, LANES), axis=0)
        proj_ref[i] = total
        square_ref[i] = squares
        return carry

    lax.fori_loop(0, count, project, 0)

    pairs = [(v, w) for v in range(nvar) for w in range(v, nvar)]
    rows = []
    for v in range(nvar):
        rows.append(sum(square_ref[s * nvar + v] for s in range(subs)))
    for v, w in pairs:
        both = sum(proj_ref[s * nvar + v] * proj_ref[s * nvar + w] for s in range(subs))
        both = sum(both[:, k : k + LANES] for k in range(0, steps, LANES))
        rows.append(jnp.sum(both.reshape(ranks // SUB, SUB, LANES), axis=0))
    nodes = counts_ref[0]
    for s in range(1, subs):
        nodes = nodes + counts_ref[s]
    tall = -(-len(rows) // SUB) * SUB
    index = lax.broadcasted_iota(jnp.int32, (tall, LANES), 0)
    lane = lax.broadcasted_iota(jnp.int32, (tall, LANES), 1)
    table = jnp.zeros((tall, LANES), jnp.float32)
    for i, row in enumerate(rows):
        table = jnp.where(index == i, jnp.sum(row, axis=0, keepdims=True), table)
    table = jnp.broadcast_to(jnp.sum(table, axis=1, keepdims=True), table.shape)
    table = jnp.sum(jnp.where(index == lane, table, 0.0), axis=0, keepdims=True)
    row = jnp.where(lane[0:1] == len(rows), nodes.astype(jnp.float32), table)
    me = x * ny + y
    row_ref[0] = row
    all_ref[me] = row
    pl.semaphore_wait(barrier, len(others))
    sent = []
    for d, other in enumerate(others):
        copy = pltpu.make_async_remote_copy(
            src_ref=row_ref.at[0],
            dst_ref=all_ref.at[me],
            send_sem=row_sems.at[0, d],
            recv_sem=row_sems.at[1, d],
            device_id=other,
            device_id_type=pl.DeviceIdType.MESH,
        )
        copy.start()
        sent.append(copy)
    for copy in sent:
        copy.wait_recv()
    total = jnp.sum(all_ref[...], axis=0)
    stat = [jnp.broadcast_to(total[:, i : i + 1], (1, LANES)) for i in range(len(rows) + 1)]
    nodes = stat[len(rows)]
    scale = [jnp.sqrt(stat[v] / (nodes * steps) + 1e-06) for v in range(nvar)]
    inverse = [1.0 / part for part in scale]
    gnorm = jnp.zeros((1, LANES), jnp.float32)
    for i, (v, w) in enumerate(pairs):
        gnorm += (1.0 if v == w else 2.0) * stat[nvar + i] * (inverse[v] * inverse[w])
    gnorm = gnorm / (nx * ny * subs * ranks * steps)
    states = []
    for s in range(subs):
        state = proj_ref[s * nvar] * inverse[0][:, 0:1]
        for v in range(1, nvar):
            state = state + proj_ref[s * nvar + v] * inverse[v][:, 0:1]
        states.append(state)
    return gnorm, states, sent


class Halo:
    def __init__(self, sizes, subs, cell_ref, sems):
        nx, ny = sizes
        x, y, at, others = everyone(sizes)
        wide = subs + 2
        self.x, self.y, self.ny, self.subs, self.wide, self.cells = x, y, ny, subs, wide, cell_ref
        self.copies = []
        sides = [(dx, dy) for dx in (-1, 0, 1) for dy in (-1, 0, 1) if dx or dy]
        for i, (dx, dy) in enumerate(sides):
            first, size = (0, subs) if dy == 0 else ((subs - 1, 1) if dy > 0 else (0, 1))
            into = (1 - dx) * wide + (1 if dy == 0 else (0 if dy > 0 else subs + 1))
            copy = pltpu.make_async_remote_copy(
                src_ref=cell_ref.at[pl.ds(wide + 1 + first, size)],
                dst_ref=cell_ref.at[pl.ds(into, size)],
                send_sem=sems.at[0, i],
                recv_sem=sems.at[1, i],
                device_id=at(dx, dy),
                device_id_type=pl.DeviceIdType.MESH,
            )
            sends = (x + dx >= 0) & (x + dx < nx) & (y + dy >= 0) & (y + dy < ny)
            takes = (x - dx >= 0) & (x - dx < nx) & (y - dy >= 0) & (y - dy < ny)
            self.copies.append((copy, sends, takes))

    def start(self, states):
        for s, state in enumerate(states):
            self.cells[self.wide + 1 + s] = state
        for copy, sends, takes in self.copies:
            pl.when(sends)(copy.start)

    def arrive(self):
        for copy, sends, takes in self.copies:
            pl.when(takes)(copy.wait_recv)

    def finish(self):
        for copy, sends, takes in self.copies:
            pl.when(sends)(copy.wait_send)

    def near(self, links_ref, s):
        columns = self.ny * self.subs
        found = []
        for b in range(links_ref.shape[1]):
            link = links_ref[s, b]
            row = link // columns
            cell = (row - self.x + 1) * self.wide + link - row * columns - self.y * self.subs + 1
            found.append(self.cells[jnp.clip(cell, 0, 3 * self.wide - 1)])
        return found


def solve_kernel(sizes, subs, nvar, counts_ref, links_ref, snaps_ref, basis_ref, out_ref, state_ref, cell_ref, f_ref, hi_ref, mid_ref, low_ref, halo_sems, *stage):
    ranks, steps = state_ref.shape[1:]
    gnorm, states, sent = gather_kernel(sizes, subs, nvar, counts_ref, snaps_ref, basis_ref, stage)
    halo = Halo(sizes, subs, cell_ref, halo_sems)
    halo.start(states)
    for s in range(subs):
        state_ref[s] = states[s]

    def near_of(s):
        return jnp.concatenate(halo.near(links_ref, s), axis=0)

    fit_body(gnorm[:, 0:1], lambda s: state_ref[s], near_of, halo.arrive, out_ref, f_ref, (hi_ref, mid_ref, low_ref),
             subs, ranks, links_ref.shape[1] * ranks, steps)
    for copy in sent:
        copy.wait_send()
    halo.finish()


def stage_shapes(devices, count, slots, ranks, steps):
    return [
        pltpu.VMEM((count, slots, steps), jnp.bfloat16),
        pltpu.VMEM((count, ranks, slots), jnp.bfloat16),
        pltpu.VMEM((count, ranks, steps), jnp.float32),
        pltpu.VMEM((count, SUB, LANES), jnp.float32),
        pltpu.VMEM((1, 1, LANES), jnp.float32),
        pltpu.VMEM((devices, 1, LANES), jnp.float32),
        pltpu.SemaphoreType.DMA((count, CHUNKS)),
        pltpu.SemaphoreType.DMA((count,)),
        pltpu.SemaphoreType.DMA((2, devices - 1)),
    ]


def solve(counts, links, snaps, basis):
    nx, ny = lax.axis_size("gx"), lax.axis_size("gy")
    subs, nvar, ranks, slots = basis.shape
    steps = snaps.shape[3]
    wide, nself, nf, full, early, rest, tall = shape_of(subs, ranks, links.shape[1] * ranks)
    smem = pl.BlockSpec(memory_space=pltpu.SMEM)
    vmem = pl.BlockSpec(memory_space=pltpu.VMEM)
    hbm = pl.BlockSpec(memory_space=pltpu.HBM)

    def kernel(*refs):
        solve_kernel((nx, ny), subs, nvar, *refs)

    return pl.pallas_call(
        kernel,
        out_shape=(
            jax.ShapeDtypeStruct((subs, ranks, nf), jnp.float32),
            jax.ShapeDtypeStruct((subs, ranks, steps), jnp.float32),
        ),
        in_specs=[smem, smem, hbm, hbm],
        out_specs=(vmem, vmem),
        scratch_shapes=[
            pltpu.VMEM((3 * (subs + 2), ranks, steps), jnp.float32),
            pltpu.VMEM((subs, tall, steps), jnp.float32),
            pltpu.VMEM((subs, tall, steps), jnp.bfloat16),
            pltpu.VMEM((subs, tall, steps), jnp.bfloat16),
            pltpu.VMEM((subs, tall, steps), jnp.bfloat16),
            pltpu.SemaphoreType.DMA((2, 8)),
        ]
        + stage_shapes(nx * ny, subs * nvar, slots, ranks, steps),
        compiler_params=pltpu.CompilerParams(collective_id=0, has_side_effects=True, vmem_limit_bytes=60 * 2**20),
        name="solve",
    )(counts, links, snaps.reshape(subs * nvar, slots, steps), basis.reshape(subs * nvar, ranks, slots))


def body(snapshots, basis, node_counts, adjacency):
    operator, states = solve(node_counts[0], adjacency[0], snapshots[0], basis[0])
    return (operator.swapaxes(1, 2)[None], states[None])


def solution(mesh):
    in_specs = (
        P("gx", "gy", None, None, None),
        P("gx", "gy", None, None, None),
        P("gx", "gy"),
        P("gx", "gy", None),
    )
    out_specs = (P("gx", "gy", None, None), P("gx", "gy", None, None))
    return jax.shard_map(body, mesh=mesh, in_specs=in_specs, out_specs=out_specs, check_vma=False)
```

```python
import jax
import jax.numpy as jnp
from jax import lax
from jax.experimental import pallas as pl
from jax.experimental.pallas import tpu as pltpu
from jax.sharding import PartitionSpec as P

beta_linear = 0.5
beta_quad = 0.5
LANES = 128
SUB = 8
STEP = 16
join = 3


def split3(a):
    hi = a.astype(jnp.bfloat16)
    left = a - hi.astype(jnp.float32)
    mid = left.astype(jnp.bfloat16)
    low = (left - mid.astype(jnp.float32)).astype(jnp.bfloat16)
    return hi, mid, low


def as_left(parts):
    hi, mid, low = parts
    return jnp.concatenate([hi, mid, hi, mid, hi, low], axis=1)


def as_right(parts, axis=1):
    hi, mid, low = parts
    return jnp.concatenate([hi, mid, mid, hi, low, hi], axis=axis)


def dot_nt(a, b):
    return lax.dot_general(a, b, (((1,), (1,)), ((), ())), preferred_element_type=jnp.float32)


def dot_nn(a, b):
    return jnp.dot(a, b, preferred_element_type=jnp.float32)


ALONG = lax.GatherDimensionNumbers(
    offset_dims=(), collapsed_slice_dims=(1,), start_index_map=(1,), operand_batching_dims=(0,), start_indices_batching_dims=(0,)
)


def pick(tile, index):
    rows = [
        lax.gather(tile[r : r + SUB], index, ALONG, (1, 1), mode=lax.GatherScatterMode.PROMISE_IN_BOUNDS)
        for r in range(0, tile.shape[0], SUB)
    ]
    return rows[0] if len(rows) == 1 else jnp.concatenate(rows, axis=0)


def whiten(block, wide):
    size = block.shape[0]
    lane8 = lax.broadcasted_iota(jnp.int32, (SUB, LANES), 1)
    half = lane8 - lane8 % wide
    lane = lax.broadcasted_iota(jnp.int32, (1, LANES), 1) % wide
    done = []
    rest = block
    for base in range(0, size, STEP):
        row = lax.broadcasted_iota(jnp.int32, (STEP, LANES), 0)
        inside = (lane >= base) & (lane < base + STEP)
        here = rest[0:STEP]
        rest = rest[STEP:]
        index = [(half + (base + j))[:, :, None] for j in range(STEP)]
        cols = jnp.stack([pick(here, index[j]) for j in range(STEP)])
        side = [pick(rest, index[j]) for j in range(STEP)] if rest.shape[0] else None
        here = jnp.where(inside, (lane - base == row).astype(jnp.float32), here)
        scaled = jnp.zeros((STEP, LANES), jnp.float32)
        for j in range(STEP):
            col = cols[0]
            inv = 1.0 / col[j : j + 1]
            now = here[j : j + 1]
            scaled = jnp.where(row == j, now * lax.rsqrt(col[j : j + 1]), scaled)
            now = now * inv
            here = jnp.where(row == j, now, here - col * now)
            if j + 1 < STEP:
                cols = cols[1:]
                top = cols[:, j : j + 1, :] * inv
                cols = jnp.where(row == j, top, cols - col * top)
        done.append(jnp.where(lane < base + STEP, scaled, 0.0))
        if rest.shape[0]:
            terms = [side[j] * here[j : j + 1] for j in range(STEP)]
            while len(terms) > 1:
                terms = [a + b for a, b in zip(terms[::2], terms[1::2])]
            rest = jnp.where(inside, 0.0, rest) - terms[0]
    return done[0] if len(done) == 1 else jnp.concatenate(done, axis=0)


def shape_of(subs, ranks, near):
    wide = LANES // subs
    nself = 1 + ranks + ranks * (ranks + 1) // 2
    nf = nself + near
    full = nf // wide
    early = nself // wide
    rest = -(-(nf - full * wide) // STEP) * STEP
    return wide, nself, nf, full, early, rest, full * wide + ranks + rest


def fit_body(gnorm, state_of, near_of, arrive, out_ref, f_ref, part_refs, subs, ranks, near, steps):
    wide, nself, nf, full, early, rest, tall = shape_of(subs, ranks, near)
    head = early * wide
    late = head + ranks
    keep = (lax.broadcasted_iota(jnp.int32, (1, steps), 1) < steps - 1).astype(jnp.float32)

    def place(s, first, size):
        for ref, part in zip(part_refs, split3(f_ref[s, first : first + size, :])):
            ref[s, first : first + size, :] = part

    tailing = []
    for s in range(subs):
        state = state_of(s)
        past = state * keep
        f_ref[s, 0:ranks, :] = past
        at = ranks
        for first in range(ranks):
            rows = past[first : first + 1] * state[first:]
            cut = max(0, min(ranks - first, head - at))
            if cut:
                f_ref[s, at : at + cut, :] = rows[:cut]
            if cut < ranks - first:
                tailing_at = at + cut - head + late
                f_ref[s, tailing_at : tailing_at + ranks - first - cut, :] = rows[cut:]
            at += ranks - first
        f_ref[s, head:late, :] = pltpu.roll(state, steps - 1, 1)
        f_ref[s, late + nself - 1 - head : late + nself - head, :] = keep
        place(s, 0, late)

    linear = beta_linear * gnorm * steps
    square = beta_quad * gnorm * gnorm * steps

    def ridge(first, size):
        row = lax.broadcasted_iota(jnp.int32, (size, LANES), 0)
        col = lax.broadcasted_iota(jnp.int32, (size, LANES), 1) % wide
        at = row + first
        level = jnp.where((at < ranks) | (at >= nself - 1), linear, square)
        level = jnp.where(at < nf, level, 1.0)
        return jnp.where(row == col, level, 0.0)

    def rows_at(j):
        return j * wide if j < early else late + (j - early) * wide

    def size_of(j):
        return wide if j < full else rest

    products = {}

    def product(rows, cols):
        if (rows, cols) not in products:
            products[rows, cols] = [
                dot_nt(
                    as_left([r[s, rows[0] : rows[1], :] for r in part_refs]),
                    as_right([r[s, cols[0] : cols[1], :] for r in part_refs]),
                )
                for s in range(subs)
            ]
        return products[rows, cols]

    group = 2 * LANES // wide

    def gram(first, size, j):
        at, span = rows_at(j), size_of(j)
        if j < early:
            block = j - j % group
            cols = (block * wide, min(block + group, early) * wide)
            rows = (cols[0], cols[0] + wide) if first < cols[0] + wide else (cols[0] + wide, late)
        else:
            cols, rows = (late, tall), (head, late)
        if first >= late:
            rows = (late, tall)
        pieces = []
        for whole in product(rows, cols):
            pieces.append(whole[first - rows[0] : first - rows[0] + size, at - cols[0] : at - cols[0] + span])
            if span < wide:
                pieces.append(jnp.zeros((size, wide - span), jnp.float32))
        return jnp.concatenate(pieces, axis=1)

    lanes = lax.broadcasted_iota(jnp.int32, (1, LANES), 1) // wide

    def pair(block):
        if block.shape[0] < wide:
            block = jnp.concatenate([block, jnp.zeros((wide - block.shape[0], LANES), block.dtype)], axis=0)
        return jnp.concatenate([jnp.where(lanes == s, block, 0.0) for s in range(subs)], axis=0)

    roots, tops, sides, lefts, boths = {}, {}, {}, {}, {}

    def extent(j, part):
        if part == 1:
            return (max(late, rows_at(j) + wide), tall)
        return (rows_at(j) + wide, late) if j < early else (head, late)

    def cut(table, k, first, last):
        part = int(first >= late)
        start = extent(k, part)[0]
        return table[k, part][first - start : last - start]

    def both(k, j):
        if (k, j) not in boths:
            block = cut(sides, k, rows_at(j), rows_at(j) + size_of(j))
            boths[k, j] = as_right(split3(pair(block)))
        return boths[k, j]

    def less(value, j, first, last, before):
        for k in before:
            value = value - dot_nt(cut(lefts, k, first, last), both(k, j))
        return value

    def top_of(j, before):
        if j not in tops:
            tops[j] = gram(rows_at(j), size_of(j), j) + ridge(j * wide, size_of(j))
        first = rows_at(j)
        tops[j] = less(tops[j], j, first, first + size_of(j), before)

    lows = {}

    def low_of(j, part, before):
        first, last = extent(j, part)
        if last > first:
            if (j, part) not in lows:
                lows[j, part] = gram(first, last - first, j)
            lows[j, part] = less(lows[j, part], j, first, last, before)

    def settle(j, part):
        if (j, part) in lows:
            side = dot_nt(as_left(split3(lows[j, part])), as_right(roots[j]))
            sides[j, part] = side
            lefts[j, part] = as_left(split3(side))

    def bring():
        for s in range(subs):
            there = near_of(s) * keep
            at = late + nself - head
            f_ref[s, at : at + near, :] = there
            f_ref[s, at + near : tall, :] = jnp.zeros((tall - at - near, steps), jnp.float32)
            place(s, late, tall - late)

    top_of(0, ())
    low_of(0, 0, ())
    for k in range(full + 1):
        if k == join:
            arrive()
        roots[k] = split3(pair(whiten(tops[k], wide)))
        if k == join:
            bring()
            for j in range(join):
                low_of(j, 1, range(j))
                settle(j, 1)
        after = k + 1 if k < full else None
        if k >= join:
            low_of(k, 1, range(k))
        if after is not None and (after < early or k >= join):
            top_of(after, range(k))
            low_of(after, 0, range(k))
        settle(k, 0)
        if k >= join:
            settle(k, 1)
        if after is not None:
            if after < early or k >= join:
                top_of(after, (k,))
                low_of(after, 0, (k,))
    answer = [None] * (full + 1)
    scaled = {}
    for key, left in lefts.items():
        scaled[key] = dot_nn(left, as_right(roots[key[0]], 0))
    for k in range(full, -1, -1):
        total = cut(scaled, k, head, late)
        for j in range(full, k, -1):
            block = cut(scaled, k, rows_at(j), rows_at(j) + size_of(j))
            total = total - dot_nn(as_left(split3(answer[j])), as_right(split3(pair(block)), 0))
        answer[k] = total
    for s in range(subs):
        def lanes_of(first, last):
            out = []
            while first < last:
                k = first // wide
                end = min(last, (k + 1) * wide)
                out.append(answer[k][:, s * wide + first - k * wide : s * wide + end - k * wide])
                first = end
            return out
        order = lanes_of(nself - 1, nself) + lanes_of(0, ranks) + lanes_of(nself, nf) + lanes_of(ranks, nself - 1)
        out_ref[s] = jnp.concatenate(order, axis=1)


CHUNKS = 1
ROWS = 16


def everyone(sizes):
    nx, ny = sizes
    x, y = lax.axis_index("gx"), lax.axis_index("gy")

    def at(dx, dy):
        return (lax.rem(x + dx + nx, nx), lax.rem(y + dy + ny, ny))

    others = [at(dx, dy) for dx in range(nx) for dy in range(ny) if dx or dy]
    return x, y, at, others


def gather_kernel(sizes, subs, nvar, counts_ref, snaps_ref, basis_ref, stage):
    nx, ny = sizes
    snap_ref, base_ref, proj_ref, square_ref, row_ref, all_ref, snap_sems, base_sems, row_sems = stage
    count, slots, steps = snap_ref.shape
    ranks = base_ref.shape[1]
    part = slots // CHUNKS
    x, y, at, others = everyone(sizes)

    def piece(i, c):
        span = pl.ds(c * part, part)
        return pltpu.make_async_copy(snaps_ref.at[i, span], snap_ref.at[i, span], snap_sems.at[i, c])

    def modes(i):
        return pltpu.make_async_copy(basis_ref.at[i], base_ref.at[i], base_sems.at[i])

    for i in range(count):
        modes(i).start()
        for c in range(CHUNKS):
            piece(i, c).start()
    barrier = pltpu.get_barrier_semaphore()
    for other in others:
        pl.semaphore_signal(barrier, inc=1, device_id=other, device_id_type=pl.DeviceIdType.MESH)

    def project(i, carry):
        live = counts_ref[i // nvar]
        modes(i).wait()
        lane = lax.broadcasted_iota(jnp.int32, (1, slots), 1)
        mask = jnp.where(lane < live, 1.0, 0.0).astype(jnp.bfloat16)
        masked = base_ref[i] * mask
        total = jnp.zeros((ranks, steps), jnp.float32)
        squares = jnp.zeros((SUB, LANES), jnp.float32)
        for c in range(CHUNKS):
            piece(i, c).wait()
            total = total + jnp.dot(
                masked[:, c * part : (c + 1) * part],
                snap_ref[i, c * part : (c + 1) * part, :],
                preferred_element_type=jnp.float32,
            )
            for first in range(c * part, (c + 1) * part, ROWS):
                value = snap_ref[i, first : first + ROWS, :].astype(jnp.float32)
                value = value * value
                value = sum(value[:, k : k + LANES] for k in range(0, steps, LANES))
                node = lax.broadcasted_iota(jnp.int32, (ROWS, LANES), 0) + first
                value = jnp.where(node < live, value, 0.0)
                squares = squares + jnp.sum(value.reshape(ROWS // SUB, SUB, LANES), axis=0)
        proj_ref[i] = total
        square_ref[i] = squares
        return carry

    lax.fori_loop(0, count, project, 0)

    pairs = [(v, w) for v in range(nvar) for w in range(v, nvar)]
    rows = []
    for v in range(nvar):
        rows.append(sum(square_ref[s * nvar + v] for s in range(subs)))
    for v, w in pairs:
        both = sum(proj_ref[s * nvar + v] * proj_ref[s * nvar + w] for s in range(subs))
        both = sum(both[:, k : k + LANES] for k in range(0, steps, LANES))
        rows.append(jnp.sum(both.reshape(ranks // SUB, SUB, LANES), axis=0))
    nodes = counts_ref[0]
    for s in range(1, subs):
        nodes = nodes + counts_ref[s]
    tall = -(-len(rows) // SUB) * SUB
    index = lax.broadcasted_iota(jnp.int32, (tall, LANES), 0)
    lane = lax.broadcasted_iota(jnp.int32, (tall, LANES), 1)
    table = jnp.zeros((tall, LANES), jnp.float32)
    for i, row in enumerate(rows):
        table = jnp.where(index == i, jnp.sum(row, axis=0, keepdims=True), table)
    table = jnp.broadcast_to(jnp.sum(table, axis=1, keepdims=True), table.shape)
    table = jnp.sum(jnp.where(index == lane, table, 0.0), axis=0, keepdims=True)
    row = jnp.where(lane[0:1] == len(rows), nodes.astype(jnp.float32), table)
    me = x * ny + y
    row_ref[0] = row
    all_ref[me] = row
    pl.semaphore_wait(barrier, len(others))
    sent = []
    for d, other in enumerate(others):
        copy = pltpu.make_async_remote_copy(
            src_ref=row_ref.at[0],
            dst_ref=all_ref.at[me],
            send_sem=row_sems.at[0, d],
            recv_sem=row_sems.at[1, d],
            device_id=other,
            device_id_type=pl.DeviceIdType.MESH,
        )
        copy.start()
        sent.append(copy)
    for copy in sent:
        copy.wait_recv()
    total = jnp.sum(all_ref[...], axis=0)
    stat = [jnp.broadcast_to(total[:, i : i + 1], (1, LANES)) for i in range(len(rows) + 1)]
    nodes = stat[len(rows)]
    scale = [jnp.sqrt(stat[v] / (nodes * steps) + 1e-06) for v in range(nvar)]
    inverse = [1.0 / part for part in scale]
    gnorm = jnp.zeros((1, LANES), jnp.float32)
    for i, (v, w) in enumerate(pairs):
        gnorm += (1.0 if v == w else 2.0) * stat[nvar + i] * (inverse[v] * inverse[w])
    gnorm = gnorm / (nx * ny * subs * ranks * steps)
    states = []
    for s in range(subs):
        state = proj_ref[s * nvar] * inverse[0][:, 0:1]
        for v in range(1, nvar):
            state = state + proj_ref[s * nvar + v] * inverse[v][:, 0:1]
        states.append(state)
    return gnorm, states, sent


class Halo:
    def __init__(self, sizes, subs, cell_ref, sems):
        nx, ny = sizes
        x, y, at, others = everyone(sizes)
        wide = subs + 2
        self.x, self.y, self.ny, self.subs, self.wide, self.cells = x, y, ny, subs, wide, cell_ref
        self.copies = []
        sides = [(dx, dy) for dx in (-1, 0, 1) for dy in (-1, 0, 1) if dx or dy]
        for i, (dx, dy) in enumerate(sides):
            first, size = (0, subs) if dy == 0 else ((subs - 1, 1) if dy > 0 else (0, 1))
            into = (1 - dx) * wide + (1 if dy == 0 else (0 if dy > 0 else subs + 1))
            copy = pltpu.make_async_remote_copy(
                src_ref=cell_ref.at[pl.ds(wide + 1 + first, size)],
                dst_ref=cell_ref.at[pl.ds(into, size)],
                send_sem=sems.at[0, i],
                recv_sem=sems.at[1, i],
                device_id=at(dx, dy),
                device_id_type=pl.DeviceIdType.MESH,
            )
            sends = (x + dx >= 0) & (x + dx < nx) & (y + dy >= 0) & (y + dy < ny)
            takes = (x - dx >= 0) & (x - dx < nx) & (y - dy >= 0) & (y - dy < ny)
            self.copies.append((copy, sends, takes))

    def start(self, states):
        for s, state in enumerate(states):
            self.cells[self.wide + 1 + s] = state
        for copy, sends, takes in self.copies:
            pl.when(sends)(copy.start)

    def arrive(self):
        for copy, sends, takes in self.copies:
            pl.when(takes)(copy.wait_recv)

    def finish(self):
        for copy, sends, takes in self.copies:
            pl.when(sends)(copy.wait_send)

    def near(self, links_ref, s):
        columns = self.ny * self.subs
        found = []
        for b in range(links_ref.shape[1]):
            link = links_ref[s, b]
            row = link // columns
            cell = (row - self.x + 1) * self.wide + link - row * columns - self.y * self.subs + 1
            found.append(self.cells[jnp.clip(cell, 0, 3 * self.wide - 1)])
        return found


def solve_kernel(sizes, subs, nvar, counts_ref, links_ref, snaps_ref, basis_ref, out_ref, state_ref, cell_ref, f_ref, hi_ref, mid_ref, low_ref, halo_sems, *stage):
    ranks, steps = state_ref.shape[1:]
    gnorm, states, sent = gather_kernel(sizes, subs, nvar, counts_ref, snaps_ref, basis_ref, stage)
    halo = Halo(sizes, subs, cell_ref, halo_sems)
    halo.start(states)
    for s in range(subs):
        state_ref[s] = states[s]

    def near_of(s):
        return jnp.concatenate(halo.near(links_ref, s), axis=0)

    fit_body(gnorm[:, 0:1], lambda s: state_ref[s], near_of, halo.arrive, out_ref, f_ref, (hi_ref, mid_ref, low_ref),
             subs, ranks, links_ref.shape[1] * ranks, steps)
    for copy in sent:
        copy.wait_send()
    halo.finish()


def stage_shapes(devices, count, slots, ranks, steps):
    return [
        pltpu.VMEM((count, slots, steps), jnp.bfloat16),
        pltpu.VMEM((count, ranks, slots), jnp.bfloat16),
        pltpu.VMEM((count, ranks, steps), jnp.float32),
        pltpu.VMEM((count, SUB, LANES), jnp.float32),
        pltpu.VMEM((1, 1, LANES), jnp.float32),
        pltpu.VMEM((devices, 1, LANES), jnp.float32),
        pltpu.SemaphoreType.DMA((count, CHUNKS)),
        pltpu.SemaphoreType.DMA((count,)),
        pltpu.SemaphoreType.DMA((2, devices - 1)),
    ]


def solve(counts, links, snaps, basis):
    nx, ny = lax.axis_size("gx"), lax.axis_size("gy")
    subs, nvar, ranks, slots = basis.shape
    steps = snaps.shape[3]
    wide, nself, nf, full, early, rest, tall = shape_of(subs, ranks, links.shape[1] * ranks)
    smem = pl.BlockSpec(memory_space=pltpu.SMEM)
    vmem = pl.BlockSpec(memory_space=pltpu.VMEM)
    hbm = pl.BlockSpec(memory_space=pltpu.HBM)

    def kernel(*refs):
        solve_kernel((nx, ny), subs, nvar, *refs)

    return pl.pallas_call(
        kernel,
        out_shape=(
            jax.ShapeDtypeStruct((subs, ranks, nf), jnp.float32),
            jax.ShapeDtypeStruct((subs, ranks, steps), jnp.float32),
        ),
        in_specs=[smem, smem, hbm, hbm],
        out_specs=(vmem, vmem),
        scratch_shapes=[
            pltpu.VMEM((3 * (subs + 2), ranks, steps), jnp.float32),
            pltpu.VMEM((subs, tall, steps), jnp.float32),
            pltpu.VMEM((subs, tall, steps), jnp.bfloat16),
            pltpu.VMEM((subs, tall, steps), jnp.bfloat16),
            pltpu.VMEM((subs, tall, steps), jnp.bfloat16),
            pltpu.SemaphoreType.DMA((2, 8)),
        ]
        + stage_shapes(nx * ny, subs * nvar, slots, ranks, steps),
        compiler_params=pltpu.CompilerParams(collective_id=0, has_side_effects=True, vmem_limit_bytes=60 * 2**20),
        name="solve",
    )(counts, links, snaps.reshape(subs * nvar, slots, steps), basis.reshape(subs * nvar, ranks, slots))


def emit_kernel(first_ref, second_ref, out_ref, kept_ref, one_ref, two_ref, sems):
    reads = [
        pltpu.make_async_copy(first_ref, one_ref, sems.at[0]),
        pltpu.make_async_copy(second_ref, two_ref, sems.at[1]),
    ]
    writes = [
        pltpu.make_async_copy(one_ref, out_ref, sems.at[2]),
        pltpu.make_async_copy(two_ref, kept_ref, sems.at[3]),
    ]
    for copy in reads:
        copy.start()
    for read, write in zip(reads, writes):
        read.wait()
        write.start()
    for copy in writes:
        copy.wait()


def emit(first, second):
    hbm = pl.BlockSpec(memory_space=pltpu.HBM)
    return pl.pallas_call(
        emit_kernel,
        out_shape=(
            jax.ShapeDtypeStruct(first.shape, first.dtype),
            jax.ShapeDtypeStruct(second.shape, second.dtype),
        ),
        in_specs=[hbm, hbm],
        out_specs=(hbm, hbm),
        scratch_shapes=[
            pltpu.VMEM(first.shape, first.dtype),
            pltpu.VMEM(second.shape, second.dtype),
            pltpu.SemaphoreType.DMA((4,)),
        ],
        name="emit",
    )(first, second)


def body(snapshots, basis, node_counts, adjacency):
    operator, states = solve(node_counts[0], adjacency[0], snapshots[0], basis[0])
    operator, states = emit(operator, states)
    return (operator.swapaxes(1, 2)[None], states[None])


def solution(mesh):
    in_specs = (
        P("gx", "gy", None, None, None),
        P("gx", "gy", None, None, None),
        P("gx", "gy"),
        P("gx", "gy", None),
    )
    out_specs = (P("gx", "gy", None, None), P("gx", "gy", None, None))
    return jax.shard_map(body, mesh=mesh, in_specs=in_specs, out_specs=out_specs, check_vma=False)
```

```python
import jax
import jax.numpy as jnp
from jax import lax
from jax.experimental import pallas as pl
from jax.experimental.pallas import tpu as pltpu
from jax.sharding import PartitionSpec as P

beta_linear = 0.5
beta_quad = 0.5
LANES = 128
SUB = 8
STEP = 16
join = 3


def split3(a):
    hi = a.astype(jnp.bfloat16)
    left = a - hi.astype(jnp.float32)
    mid = left.astype(jnp.bfloat16)
    low = (left - mid.astype(jnp.float32)).astype(jnp.bfloat16)
    return hi, mid, low


def as_left(parts):
    hi, mid, low = parts
    return jnp.concatenate([hi, mid, hi, mid, hi, low], axis=1)


def as_right(parts, axis=1):
    hi, mid, low = parts
    return jnp.concatenate([hi, mid, mid, hi, low, hi], axis=axis)


def dot_nt(a, b):
    return lax.dot_general(a, b, (((1,), (1,)), ((), ())), preferred_element_type=jnp.float32)


def dot_nn(a, b):
    return jnp.dot(a, b, preferred_element_type=jnp.float32)


ALONG = lax.GatherDimensionNumbers(
    offset_dims=(), collapsed_slice_dims=(1,), start_index_map=(1,), operand_batching_dims=(0,), start_indices_batching_dims=(0,)
)


def pick(tile, index):
    rows = [
        lax.gather(tile[r : r + SUB], index, ALONG, (1, 1), mode=lax.GatherScatterMode.PROMISE_IN_BOUNDS)
        for r in range(0, tile.shape[0], SUB)
    ]
    return rows[0] if len(rows) == 1 else jnp.concatenate(rows, axis=0)


def whiten(block, wide):
    size = block.shape[0]
    lane8 = lax.broadcasted_iota(jnp.int32, (SUB, LANES), 1)
    half = lane8 - lane8 % wide
    lane = lax.broadcasted_iota(jnp.int32, (1, LANES), 1) % wide
    done = []
    rest = block
    for base in range(0, size, STEP):
        row = lax.broadcasted_iota(jnp.int32, (STEP, LANES), 0)
        inside = (lane >= base) & (lane < base + STEP)
        here = rest[0:STEP]
        rest = rest[STEP:]
        index = [(half + (base + j))[:, :, None] for j in range(STEP)]
        cols = jnp.stack([pick(here, index[j]) for j in range(STEP)])
        side = [pick(rest, index[j]) for j in range(STEP)] if rest.shape[0] else None
        here = jnp.where(inside, (lane - base == row).astype(jnp.float32), here)
        scaled = jnp.zeros((STEP, LANES), jnp.float32)
        for j in range(STEP):
            col = cols[0]
            inv = 1.0 / col[j : j + 1]
            now = here[j : j + 1]
            scaled = jnp.where(row == j, now * lax.rsqrt(col[j : j + 1]), scaled)
            now = now * inv
            here = jnp.where(row == j, now, here - col * now)
            if j + 1 < STEP:
                cols = cols[1:]
                top = cols[:, j : j + 1, :] * inv
                cols = jnp.where(row == j, top, cols - col * top)
        done.append(jnp.where(lane < base + STEP, scaled, 0.0))
        if rest.shape[0]:
            terms = [side[j] * here[j : j + 1] for j in range(STEP)]
            while len(terms) > 1:
                terms = [a + b for a, b in zip(terms[::2], terms[1::2])]
            rest = jnp.where(inside, 0.0, rest) - terms[0]
    return done[0] if len(done) == 1 else jnp.concatenate(done, axis=0)


def shape_of(subs, ranks, near):
    wide = LANES // subs
    nself = 1 + ranks + ranks * (ranks + 1) // 2
    nf = nself + near
    full = nf // wide
    early = nself // wide
    rest = -(-(nf - full * wide) // STEP) * STEP
    return wide, nself, nf, full, early, rest, full * wide + -(-ranks // STEP) * STEP + rest


def fit_body(gnorm, state_of, near_of, arrive, out_ref, f_ref, part_refs, subs, ranks, near, steps):
    wide, nself, nf, full, early, rest, tall = shape_of(subs, ranks, near)
    head = early * wide
    late = head + -(-ranks // STEP) * STEP
    keep = (lax.broadcasted_iota(jnp.int32, (1, steps), 1) < steps - 1).astype(jnp.float32)

    def place(s, first, size):
        for ref, part in zip(part_refs, split3(f_ref[s, first : first + size, :])):
            ref[s, first : first + size, :] = part

    tailing = []
    for s in range(subs):
        state = state_of(s)
        past = state * keep
        f_ref[s, 0:ranks, :] = past
        at = ranks
        for first in range(ranks):
            rows = past[first : first + 1] * state[first:]
            cut = max(0, min(ranks - first, head - at))
            if cut:
                f_ref[s, at : at + cut, :] = rows[:cut]
            if cut < ranks - first:
                tailing_at = at + cut - head + late
                f_ref[s, tailing_at : tailing_at + ranks - first - cut, :] = rows[cut:]
            at += ranks - first
        f_ref[s, head : head + ranks, :] = pltpu.roll(state, steps - 1, 1)
        if late > head + ranks:
            f_ref[s, head + ranks : late, :] = jnp.zeros((late - head - ranks, steps), jnp.float32)
        f_ref[s, late + nself - 1 - head : late + nself - head, :] = keep
        place(s, 0, late)

    linear = beta_linear * gnorm * steps
    square = beta_quad * gnorm * gnorm * steps

    def ridge(first, size):
        row = lax.broadcasted_iota(jnp.int32, (size, LANES), 0)
        col = lax.broadcasted_iota(jnp.int32, (size, LANES), 1) % wide
        at = row + first
        level = jnp.where((at < ranks) | (at >= nself - 1), linear, square)
        level = jnp.where(at < nf, level, 1.0)
        return jnp.where(row == col, level, 0.0)

    def rows_at(j):
        return j * wide if j < early else late + (j - early) * wide

    def size_of(j):
        return wide if j < full else rest

    products = {}

    def product(rows, cols):
        if (rows, cols) not in products:
            products[rows, cols] = [
                dot_nt(
                    as_left([r[s, rows[0] : rows[1], :] for r in part_refs]),
                    as_right([r[s, cols[0] : cols[1], :] for r in part_refs]),
                )
                for s in range(subs)
            ]
        return products[rows, cols]

    group = 2 * LANES // wide

    def gram(first, size, j):
        at, span = rows_at(j), size_of(j)
        if j < early:
            block = j - j % group
            cols = (block * wide, min(block + group, early) * wide)
            rows = (cols[0], cols[0] + wide) if first < cols[0] + wide else (cols[0] + wide, late)
        else:
            cols, rows = (late, tall), (head, late)
        if first >= late:
            rows = (late, tall)
        pieces = []
        for whole in product(rows, cols):
            pieces.append(whole[first - rows[0] : first - rows[0] + size, at - cols[0] : at - cols[0] + span])
            if span < wide:
                pieces.append(jnp.zeros((size, wide - span), jnp.float32))
        return jnp.concatenate(pieces, axis=1)

    lanes = lax.broadcasted_iota(jnp.int32, (1, LANES), 1) // wide

    def pair(block):
        if block.shape[0] < wide:
            block = jnp.concatenate([block, jnp.zeros((wide - block.shape[0], LANES), block.dtype)], axis=0)
        return jnp.concatenate([jnp.where(lanes == s, block, 0.0) for s in range(subs)], axis=0)

    roots, sides, lefts, boths, cols, tops, heads = {}, {}, {}, {}, {}, {}, {}

    def extent(j, part):
        if part == 1:
            return (max(late, rows_at(j)), tall)
        return (rows_at(j), late) if j < early else (head, late)

    def home(j):
        return 0 if j < early else 1

    def after(k, part):
        first, last = extent(k, part)
        return (first + size_of(k), last) if part == home(k) else (first, last)

    def left_of(k, parts):
        if (k, parts) not in lefts:
            have = [sides[k, p] for p in parts if (k, p) in sides]
            lefts[k, parts] = as_left(split3(have[0] if len(have) == 1 else jnp.concatenate(have, axis=0)))
        return lefts[k, parts]

    def index(k, parts, row):
        base = 0
        for p in parts:
            first, last = after(k, p)
            if first <= row < last:
                return base + row - first
            base += last - first

    def both(k, j):
        if (k, j) not in boths:
            at = index(k, (home(j),), rows_at(j))
            boths[k, j] = as_right(split3(pair(sides[k, home(j)][at : at + size_of(j)])))
        return boths[k, j]

    def start(j, parts):
        for part in parts:
            if part == home(j):
                tops[j] = gram(rows_at(j), size_of(j), j) + ridge(j * wide, size_of(j))
            first, last = after(j, part)
            if last > first:
                cols[j, part] = gram(first, last - first, j)

    def update(j, before, parts):
        for k in before:
            ahead = j == k + 1 and home(j) in parts
            if ahead:
                tops[j] = tops[j] - dot_nt(as_left(split3(heads[k])), both(k, j))
            wanted = [after(j, p) for p in parts]
            if home(j) in parts and not ahead:
                wanted.append((rows_at(j), rows_at(j) + size_of(j)))
            wanted = [w for w in wanted if w[1] > w[0]]
            if not wanted:
                continue
            base = min(index(k, parts, w[0]) for w in wanted)
            less = dot_nt(left_of(k, parts)[base:], both(k, j))
            for part in parts:
                low, high = after(j, part)
                if high > low:
                    at = index(k, parts, low) - base
                    cols[j, part] = cols[j, part] - less[at : at + high - low]
                if part == home(j) and not ahead:
                    at = index(k, parts, rows_at(j)) - base
                    tops[j] = tops[j] - less[at : at + size_of(j)]

    def settle(k, parts):
        lead = k < full and home(k + 1) in parts
        rest = []
        for part in parts:
            if (k, part) in cols:
                value = cols[k, part]
                if lead and part == home(k + 1):
                    size = size_of(k + 1)
                    heads[k] = dot_nt(as_left(split3(value[:size])), as_right(roots[k]))
                    boths[k, k + 1] = as_right(split3(pair(heads[k])))
                    value = value[size:]
                if value.shape[0]:
                    rest.append((part, value))
        done = {}
        if rest:
            value = rest[0][1] if len(rest) == 1 else jnp.concatenate([v for p, v in rest], axis=0)
            side = dot_nt(as_left(split3(value)), as_right(roots[k]))
            at = 0
            for part, value in rest:
                done[part] = side[at : at + value.shape[0]]
                at += value.shape[0]
        for part in parts:
            pieces = [heads[k]] if lead and part == home(k + 1) else []
            if part in done:
                pieces.append(done[part])
            if pieces:
                sides[k, part] = pieces[0] if len(pieces) == 1 else jnp.concatenate(pieces, axis=0)

    def bring():
        for s in range(subs):
            there = near_of(s) * keep
            at = late + nself - head
            f_ref[s, at : at + near, :] = there
            f_ref[s, at + near : tall, :] = jnp.zeros((tall - at - near, steps), jnp.float32)
            place(s, late, tall - late)

    start(0, (0,))
    for k in range(full + 1):
        if k == join:
            arrive()
        roots[k] = split3(pair(whiten(tops[k], wide)))
        if k == join:
            bring()
            for j in range(join + 1):
                start(j, (1,))
                update(j, range(j), (1,))
                if j < join:
                    settle(j, (1,))
        parts = (0,) if k < join else (0, 1)
        if k < full:
            start(k + 1, parts)
            update(k + 1, range(k), parts)
        settle(k, parts)
        if k < full:
            update(k + 1, (k,), parts)
    answer = [None] * (full + 1)
    scaled = [dot_nn(left_of(k, (0, 1)), as_right(roots[k], 0)) for k in range(full + 1)]
    for k in range(full, -1, -1):
        at = index(k, (0, 1), head)
        total = scaled[k][at : at + ranks]
        for j in range(full, k, -1):
            at = index(k, (0, 1), rows_at(j))
            block = scaled[k][at : at + size_of(j)]
            total = total - dot_nn(as_left(split3(answer[j])), as_right(split3(pair(block)), 0))
        answer[k] = total
    for s in range(subs):
        def lanes_of(first, last):
            out = []
            while first < last:
                k = first // wide
                end = min(last, (k + 1) * wide)
                out.append(answer[k][:, s * wide + first - k * wide : s * wide + end - k * wide])
                first = end
            return out
        order = lanes_of(nself - 1, nself) + lanes_of(0, ranks) + lanes_of(nself, nf) + lanes_of(ranks, nself - 1)
        out_ref[s] = jnp.concatenate(order, axis=1)


CHUNKS = 1
ROWS = 16


def everyone(sizes):
    nx, ny = sizes
    x, y = lax.axis_index("gx"), lax.axis_index("gy")

    def at(dx, dy):
        return (lax.rem(x + dx + nx, nx), lax.rem(y + dy + ny, ny))

    others = [at(dx, dy) for dx in range(nx) for dy in range(ny) if dx or dy]
    return x, y, at, others


def gather_kernel(sizes, subs, nvar, counts_ref, snaps_ref, basis_ref, small, stage):
    nx, ny = sizes
    snap_ref, base_ref, proj_ref, square_ref, row_ref, all_ref, snap_sems, base_sems, row_sems = stage
    count, slots, steps = snap_ref.shape
    ranks = base_ref.shape[1]
    part = slots // CHUNKS
    x, y, at, others = everyone(sizes)

    def piece(i, c):
        span = pl.ds(c * part, part)
        return pltpu.make_async_copy(snaps_ref.at[i, span], snap_ref.at[i, span], snap_sems.at[i, c])

    def modes(i):
        return pltpu.make_async_copy(basis_ref.at[i], base_ref.at[i], base_sems.at[i])

    for i in range(count):
        if i == 1:
            for copy in small:
                copy.start()
        modes(i).start()
        for c in range(CHUNKS):
            piece(i, c).start()
    barrier = pltpu.get_barrier_semaphore()
    for other in others:
        pl.semaphore_signal(barrier, inc=1, device_id=other, device_id_type=pl.DeviceIdType.MESH)

    def project(i, carry):
        live = counts_ref[i // nvar]
        modes(i).wait()
        lane = lax.broadcasted_iota(jnp.int32, (1, slots), 1)
        mask = jnp.where(lane < live, 1.0, 0.0).astype(jnp.bfloat16)
        masked = base_ref[i] * mask
        total = jnp.zeros((ranks, steps), jnp.float32)
        squares = jnp.zeros((SUB, LANES), jnp.float32)
        for c in range(CHUNKS):
            piece(i, c).wait()
            for first in range(c * part, (c + 1) * part, ROWS):
                value = snap_ref[i, first : first + ROWS, :].astype(jnp.float32)
                value = value * value
                value = sum(value[:, k : k + LANES] for k in range(0, steps, LANES))
                node = lax.broadcasted_iota(jnp.int32, (ROWS, LANES), 0) + first
                value = jnp.where(node < live, value, 0.0)
                squares = squares + jnp.sum(value.reshape(ROWS // SUB, SUB, LANES), axis=0)
            total = total + jnp.dot(
                masked[:, c * part : (c + 1) * part],
                snap_ref[i, c * part : (c + 1) * part, :],
                preferred_element_type=jnp.float32,
            )
        proj_ref[i] = total
        square_ref[i] = squares
        return carry

    for copy in small:
        copy.wait()
    lax.fori_loop(0, count, project, 0)

    pairs = [(v, w) for v in range(nvar) for w in range(v, nvar)]
    rows = []
    for v in range(nvar):
        rows.append(sum(square_ref[s * nvar + v] for s in range(subs)))
    for v, w in pairs:
        both = sum(proj_ref[s * nvar + v] * proj_ref[s * nvar + w] for s in range(subs))
        both = sum(both[:, k : k + LANES] for k in range(0, steps, LANES))
        rows.append(jnp.sum(both.reshape(ranks // SUB, SUB, LANES), axis=0))
    nodes = counts_ref[0]
    for s in range(1, subs):
        nodes = nodes + counts_ref[s]
    tall = -(-len(rows) // SUB) * SUB
    index = lax.broadcasted_iota(jnp.int32, (tall, LANES), 0)
    lane = lax.broadcasted_iota(jnp.int32, (tall, LANES), 1)
    table = jnp.zeros((tall, LANES), jnp.float32)
    for i, row in enumerate(rows):
        table = jnp.where(index == i, jnp.sum(row, axis=0, keepdims=True), table)
    table = jnp.broadcast_to(jnp.sum(table, axis=1, keepdims=True), table.shape)
    table = jnp.sum(jnp.where(index == lane, table, 0.0), axis=0, keepdims=True)
    row = jnp.where(lane[0:1] == len(rows), nodes.astype(jnp.float32), table)
    me = x * ny + y
    row_ref[0] = row
    all_ref[me] = row
    pl.semaphore_wait(barrier, len(others))
    sent = []
    for d, other in enumerate(others):
        copy = pltpu.make_async_remote_copy(
            src_ref=row_ref.at[0],
            dst_ref=all_ref.at[me],
            send_sem=row_sems.at[0, d],
            recv_sem=row_sems.at[1, d],
            device_id=other,
            device_id_type=pl.DeviceIdType.MESH,
        )
        copy.start()
        sent.append(copy)
    for copy in sent:
        copy.wait_recv()
    total = jnp.sum(all_ref[...], axis=0)
    stat = [jnp.broadcast_to(total[:, i : i + 1], (1, LANES)) for i in range(len(rows) + 1)]
    nodes = stat[len(rows)]
    scale = [jnp.sqrt(stat[v] / (nodes * steps) + 1e-06) for v in range(nvar)]
    inverse = [1.0 / part for part in scale]
    gnorm = jnp.zeros((1, LANES), jnp.float32)
    for i, (v, w) in enumerate(pairs):
        gnorm += (1.0 if v == w else 2.0) * stat[nvar + i] * (inverse[v] * inverse[w])
    gnorm = gnorm / (nx * ny * subs * ranks * steps)
    states = []
    for s in range(subs):
        state = proj_ref[s * nvar] * inverse[0][:, 0:1]
        for v in range(1, nvar):
            state = state + proj_ref[s * nvar + v] * inverse[v][:, 0:1]
        states.append(state)
    return gnorm, states, sent


class Halo:
    def __init__(self, sizes, subs, cell_ref, sems):
        nx, ny = sizes
        x, y, at, others = everyone(sizes)
        wide = subs + 2
        self.x, self.y, self.ny, self.subs, self.wide, self.cells = x, y, ny, subs, wide, cell_ref
        self.copies = []
        sides = [(dx, dy) for dx in (-1, 0, 1) for dy in (-1, 0, 1) if dx or dy]
        for i, (dx, dy) in enumerate(sides):
            first, size = (0, subs) if dy == 0 else ((subs - 1, 1) if dy > 0 else (0, 1))
            into = (1 - dx) * wide + (1 if dy == 0 else (0 if dy > 0 else subs + 1))
            copy = pltpu.make_async_remote_copy(
                src_ref=cell_ref.at[pl.ds(wide + 1 + first, size)],
                dst_ref=cell_ref.at[pl.ds(into, size)],
                send_sem=sems.at[0, i],
                recv_sem=sems.at[1, i],
                device_id=at(dx, dy),
                device_id_type=pl.DeviceIdType.MESH,
            )
            sends = (x + dx >= 0) & (x + dx < nx) & (y + dy >= 0) & (y + dy < ny)
            takes = (x - dx >= 0) & (x - dx < nx) & (y - dy >= 0) & (y - dy < ny)
            self.copies.append((copy, sends, takes))

    def start(self, states):
        for s, state in enumerate(states):
            self.cells[self.wide + 1 + s] = state
        for copy, sends, takes in self.copies:
            pl.when(sends)(copy.start)

    def arrive(self):
        for copy, sends, takes in self.copies:
            pl.when(takes)(copy.wait_recv)

    def finish(self):
        for copy, sends, takes in self.copies:
            pl.when(sends)(copy.wait_send)

    def near(self, links_ref, s):
        columns = self.ny * self.subs
        found = []
        for b in range(links_ref.shape[1]):
            link = links_ref[s, b]
            row = link // columns
            cell = (row - self.x + 1) * self.wide + link - row * columns - self.y * self.subs + 1
            found.append(self.cells[jnp.clip(cell, 0, 3 * self.wide - 1)])
        return found


def solve_kernel(sizes, subs, nvar, far_counts_ref, far_links_ref, snaps_ref, basis_ref, out_ref, state_ref, counts_ref, links_ref, small_sems, cell_ref, f_ref, hi_ref, mid_ref, low_ref, halo_sems, *stage):
    ranks, steps = state_ref.shape[1:]
    small = [
        pltpu.make_async_copy(far_counts_ref, counts_ref, small_sems.at[0]),
        pltpu.make_async_copy(far_links_ref, links_ref, small_sems.at[1]),
    ]
    gnorm, states, sent = gather_kernel(sizes, subs, nvar, counts_ref, snaps_ref, basis_ref, small, stage)
    halo = Halo(sizes, subs, cell_ref, halo_sems)
    halo.start(states)
    for s in range(subs):
        state_ref[s] = states[s]

    def near_of(s):
        return jnp.concatenate(halo.near(links_ref, s), axis=0)

    fit_body(gnorm[:, 0:1], lambda s: state_ref[s], near_of, halo.arrive, out_ref, f_ref, (hi_ref, mid_ref, low_ref),
             subs, ranks, links_ref.shape[1] * ranks, steps)
    for copy in sent:
        copy.wait_send()
    halo.finish()


def stage_shapes(devices, count, slots, ranks, steps):
    return [
        pltpu.VMEM((count, slots, steps), jnp.bfloat16),
        pltpu.VMEM((count, ranks, slots), jnp.bfloat16),
        pltpu.VMEM((count, ranks, steps), jnp.float32),
        pltpu.VMEM((count, SUB, LANES), jnp.float32),
        pltpu.VMEM((1, 1, LANES), jnp.float32),
        pltpu.VMEM((devices, 1, LANES), jnp.float32),
        pltpu.SemaphoreType.DMA((count, CHUNKS)),
        pltpu.SemaphoreType.DMA((count,)),
        pltpu.SemaphoreType.DMA((2, devices - 1)),
    ]


def solve(counts, links, snaps, basis):
    nx, ny = lax.axis_size("gx"), lax.axis_size("gy")
    subs, nvar, ranks, slots = basis.shape
    steps = snaps.shape[3]
    wide, nself, nf, full, early, rest, tall = shape_of(subs, ranks, links.shape[1] * ranks)
    vmem = pl.BlockSpec(memory_space=pltpu.VMEM)
    hbm = pl.BlockSpec(memory_space=pltpu.HBM)

    def kernel(*refs):
        solve_kernel((nx, ny), subs, nvar, *refs)

    return pl.pallas_call(
        kernel,
        out_shape=(
            jax.ShapeDtypeStruct((subs, ranks, nf), jnp.float32),
            jax.ShapeDtypeStruct((subs, ranks, steps), jnp.float32),
        ),
        in_specs=[hbm, hbm, hbm, hbm],
        out_specs=(vmem, vmem),
        scratch_shapes=[
            pltpu.SMEM(counts.shape, jnp.int32),
            pltpu.SMEM(links.shape, jnp.int32),
            pltpu.SemaphoreType.DMA((2,)),
            pltpu.VMEM((3 * (subs + 2), ranks, steps), jnp.float32),
            pltpu.VMEM((subs, tall, steps), jnp.float32),
            pltpu.VMEM((subs, tall, steps), jnp.bfloat16),
            pltpu.VMEM((subs, tall, steps), jnp.bfloat16),
            pltpu.VMEM((subs, tall, steps), jnp.bfloat16),
            pltpu.SemaphoreType.DMA((2, 8)),
        ]
        + stage_shapes(nx * ny, subs * nvar, slots, ranks, steps),
        compiler_params=pltpu.CompilerParams(collective_id=0, has_side_effects=True, vmem_limit_bytes=60 * 2**20),
        name="solve",
    )(counts, links, snaps.reshape(subs * nvar, slots, steps), basis.reshape(subs * nvar, ranks, slots))


def emit_kernel(first_ref, second_ref, out_ref, kept_ref, one_ref, two_ref, sems):
    reads = [
        pltpu.make_async_copy(first_ref, one_ref, sems.at[0]),
        pltpu.make_async_copy(second_ref, two_ref, sems.at[1]),
    ]
    writes = [
        pltpu.make_async_copy(one_ref, out_ref, sems.at[2]),
        pltpu.make_async_copy(two_ref, kept_ref, sems.at[3]),
    ]
    for copy in reads:
        copy.start()
    for read, write in zip(reads, writes):
        read.wait()
        write.start()
    for copy in writes:
        copy.wait()


def emit(first, second):
    hbm = pl.BlockSpec(memory_space=pltpu.HBM)
    return pl.pallas_call(
        emit_kernel,
        out_shape=(
            jax.ShapeDtypeStruct(first.shape, first.dtype),
            jax.ShapeDtypeStruct(second.shape, second.dtype),
        ),
        in_specs=[hbm, hbm],
        out_specs=(hbm, hbm),
        scratch_shapes=[
            pltpu.VMEM(first.shape, first.dtype),
            pltpu.VMEM(second.shape, second.dtype),
            pltpu.SemaphoreType.DMA((4,)),
        ],
        name="emit",
    )(first, second)


def body(snapshots, basis, node_counts, adjacency):
    operator, states = solve(node_counts[0], adjacency[0], snapshots[0], basis[0])
    operator, states = emit(operator, states)
    return (operator.swapaxes(1, 2)[None], states[None])


def solution(mesh):
    in_specs = (
        P("gx", "gy", None, None, None),
        P("gx", "gy", None, None, None),
        P("gx", "gy"),
        P("gx", "gy", None),
    )
    out_specs = (P("gx", "gy", None, None), P("gx", "gy", None, None))
    return jax.shard_map(body, mesh=mesh, in_specs=in_specs, out_specs=out_specs, check_vma=False)
```
